8 devices in a mesh: rep: 1 (over z), tp: 2 (over y), dp: 4 (over x, core).
Axes of the slice: x: 2, y: 2, z: 1, core: 2. Of those that a mesh axis runs over, the one named last changes fastest.
Arguments:
- grad_partial: float32 [4, 24, 2048, 768], P(('rep', 'dp'), None, None, 'tp')
- momentum: float32 [24, 2048, 768], P('rep', 'dp', 'tp')
- weight: float32 [24, 2048, 768], P('rep', 'dp', 'tp')
- learn_rate: float32 [24], P('rep')
- decay_rate: float32 [], replicated
Outputs:
- output 1: float32 [24, 2048, 768], P('rep', 'dp', 'tp')
- output 2: float32 [24, 2048, 768], P('rep', 'dp', 'tp')
- output 3: bfloat16 [24, 2048, 768], P('rep', None, 'tp')
All inputs are finite; a program needn't handle non-finite values.
Results may differ from the reference program's by a relative error of at most 0.0130496.
Values are sent between devices in bfloat16 or wider.
A program may use at most 1 GiB of HBM per device.

```python
import math
import jax
import jax.numpy as jnp
from jax import lax

DP_SIZE = 4
MATS = 24
ROWS = 2048
COLS = 768

MOMENTUM = 0.95
NS_STEPS = 5
COEF_A = 3.4445
COEF_B = -4.7750
COEF_C = 2.0315
NORM_EPS = 1e-7
OUT_SCALE = 0.2 * math.sqrt(max(ROWS, COLS))


def setup_inputs(seed: int = 0, part: int = 0) -> dict:
    part_key = jax.random.fold_in(jax.random.key(seed), part)
    key_grad, key_scale, key_mom, key_weight, key_rate = jax.random.split(part_key, 5)
    key_decay = jax.random.key(seed + 1)
    dev_scale = jax.random.uniform(key_scale, (DP_SIZE, 1, 1, 1), minval=0.5, maxval=2.0)
    grad_partial = jax.random.normal(key_grad, (DP_SIZE, MATS, ROWS, COLS)) * dev_scale * math.sqrt(DP_SIZE)
    momentum = jax.random.normal(key_mom, (MATS, ROWS, COLS))
    weight = 0.25 * jax.random.normal(key_weight, (MATS, ROWS, COLS))
    learn_rate = jax.random.uniform(key_rate, (MATS,), minval=0.1, maxval=1.0)
    decay_rate = jax.random.uniform(key_decay, (), minval=0.2, maxval=0.5)
    return {
        "grad_partial": grad_partial.astype(jnp.float32),
        "momentum": momentum.astype(jnp.float32),
        "weight": weight.astype(jnp.float32),
        "learn_rate": learn_rate.astype(jnp.float32),
        "decay_rate": decay_rate.astype(jnp.float32),
    }


def orthogonalize(update):
    upd_f32 = update.astype(jnp.float32)
    norm_val = jnp.sqrt(jnp.sum(upd_f32 * upd_f32))
    x_cur = (upd_f32 / (norm_val + NORM_EPS)).astype(jnp.bfloat16)
    if ROWS > COLS:
        x_cur = x_cur.T
    for step_idx in range(NS_STEPS):
        gram_mat = jnp.dot(x_cur, x_cur.T, preferred_element_type=jnp.float32).astype(jnp.bfloat16)
        gram_sq = jnp.dot(gram_mat, gram_mat, preferred_element_type=jnp.float32)
        poly_mat = (COEF_B * gram_mat.astype(jnp.float32) + COEF_C * gram_sq).astype(jnp.bfloat16)
        prod_mat = jnp.dot(poly_mat, x_cur, preferred_element_type=jnp.float32)
        x_cur = (COEF_A * x_cur.astype(jnp.float32) + prod_mat).astype(jnp.bfloat16)
    if ROWS > COLS:
        x_cur = x_cur.T
    return x_cur


def reference(grad_partial, momentum, weight, learn_rate, decay_rate):
    grad_mean = jnp.mean(grad_partial, axis=0)
    mom_new = MOMENTUM * momentum + grad_mean
    update = (grad_mean + MOMENTUM * mom_new).astype(jnp.bfloat16)
    ortho_mat = lax.map(orthogonalize, update)
    rate_col = learn_rate[:, None, None]
    weight_new = weight - rate_col * (OUT_SCALE * ortho_mat.astype(jnp.float32) + decay_rate * weight)
    return mom_new, weight_new, weight_new.astype(jnp.bfloat16)
```

```python
import functools
import math

import jax
import jax.numpy as jnp
from jax import lax
from jax.experimental import pallas as pl
from jax.experimental.pallas import tpu as pltpu
from jax.sharding import PartitionSpec as P

MOMENTUM = 0.95
NS_STEPS = 5
COEF_A = 3.4445
COEF_B = -4.7750
COEF_C = 2.0315
NORM_EPS = 1e-7

MESH = pl.DeviceIdType.MESH
F32 = jnp.float32
BF16 = jnp.bfloat16

MATS = 24
ROWS = 2048
COLS = 768
DEVS = 8
ROUNDS = MATS // DEVS
RB = ROWS // 4
CB = COLS // 2
OUT_SCALE = 0.2 * math.sqrt(max(ROWS, COLS))

LAG = 3
LEAD = 2
A_SLOTS = 2 * LEAD
B_SLOTS = 2 * LAG
NS_START = (8 + LAG + 2, 16 + LAG + 2, 24 + LAG)
W_START = (NS_START[0] + 7, NS_START[2], NS_START[2] + 5)
STEPS = NS_START[2] + 6
CHUNK = 64


def rem(a, b):
    return lax.rem(a, b)


def row_loop(total, body):
    @pl.loop(0, total // CHUNK)
    def _(i):
        body(pl.ds(pl.multiple_of(i * CHUNK, CHUNK), CHUNK))


def kernel(
    grad, mom, wt, rate, decay,
    mom_o, wt_o, wb_o,
    own, ra, sendb, recvb, acc, momi, momq, wti, wtq, ust, wst, xb, rx, gram, poly,
    own_sem, a_send, a_recv, rs_send, rs_recv, momi_sem, momq_sem, wti_sem, wtq_sem,
    u_send, u_recv, x_send, x_recv, w_loc, w_par, w_nbr, wp_recv, wx_recv, f_send, f_recv,
):
    dp = lax.axis_index("dp")
    y = lax.axis_index("tp")
    x = lax.div(dp, 2)
    c = rem(dp, 2)
    me = y * 4 + dp
    partner = {"tp": y, "dp": x * 2 + (1 - c)}
    nbr_dp = (1 - x) * 2 + c
    nbr = {"tp": y, "dp": nbr_dp}

    def coords(i):
        dx, dy, dc = lax.div(i, 4), rem(lax.div(i, 2), 2), rem(i, 2)
        yy = rem(y + dy, 2)
        dd = rem(x + dx, 2) * 2 + rem(c + dc, 2)
        return yy, dd

    def remote(src, dst, ss, rs, dev):
        return pltpu.make_async_remote_copy(
            src_ref=src, dst_ref=dst, send_sem=ss, recv_sem=rs, device_id=dev, device_id_type=MESH
        )

    def xblock(r, dd, yy):
        return xb.at[
            r, pl.ds(pl.multiple_of(dd * RB, RB), RB), pl.ds(pl.multiple_of(yy * CB, CB), CB)
        ]

    def own_copy(t):
        s = rem(t, 2)
        return pltpu.make_async_copy(grad.at[t, :, c], own.at[s], own_sem.at[s])

    def a_copy(t):
        s = rem(t, A_SLOTS)
        return remote(grad.at[t, :, 1 - c], ra.at[s], a_send.at[s], a_recv.at[s], partner)

    def rs_copy(t):
        s, d = rem(t, LAG), rem(t, B_SLOTS)
        return remote(sendb.at[s], recvb.at[d], rs_send.at[s], rs_recv.at[d], nbr)

    def mom_load(j):
        s = rem(j, 2)
        return pltpu.make_async_copy(mom.at[j], momi.at[s], momi_sem.at[s])

    def mom_store(j):
        s = rem(j, 2)
        return pltpu.make_async_copy(momq.at[s], mom_o.at[j], momq_sem.at[s])

    def u_copy(j):
        k = rem(j, DEVS)
        r = lax.div(j, DEVS)
        dev = {"tp": lax.div(k, 4), "dp": rem(k, 4)}
        return remote(ust.at[k], xblock(r, dp, y), u_send.at[k], u_recv.at[r * DEVS + me], dev)

    def x_copy(r, i):
        yy, dd = coords(i)
        j = r * DEVS + me
        return remote(
            xblock(r, dd, yy), rx.at[j], x_send.at[r * DEVS + i], x_recv.at[j], {"tp": yy, "dp": dd}
        )

    def w_mat(w):
        yy, dd = coords(rem(w, DEVS))
        return lax.div(w, DEVS) * DEVS + yy * 4 + dd

    def wt_load(w):
        s = rem(w, 2)
        return pltpu.make_async_copy(wt.at[w_mat(w)], wti.at[s], wti_sem.at[s])

    def wt_store(w):
        s = rem(w, 2)
        return pltpu.make_async_copy(wtq.at[s], wt_o.at[w_mat(w)], wtq_sem.at[s])

    def w_copies(w):
        j, s = w_mat(w), rem(w, DEVS)
        dst = wb_o.at[j, dp]
        return (
            pltpu.make_async_copy(wst.at[s], dst, w_loc.at[s]),
            remote(wst.at[s], dst, w_par.at[s], wp_recv.at[j], partner),
            remote(wst.at[s], dst, w_nbr.at[s], wx_recv.at[j], nbr),
        )

    def f_mat(w):
        i = rem(w, DEVS)
        dx, dy, dc = lax.div(i, 4), rem(lax.div(i, 2), 2), rem(i, 2)
        dd = rem(1 - x + dx, 2) * 2 + rem(c + dc, 2)
        return lax.div(w, DEVS) * DEVS + rem(y + dy, 2) * 4 + dd

    def f_copy(w):
        j = f_mat(w)
        ref = wb_o.at[j, nbr_dp]
        return remote(ref, ref, f_send.at[j], f_recv.at[j], partner)

    def presum(t):
        own_copy(t).wait()
        a_copy(t).wait_recv()

        @pl.when(t >= LAG)
        def _():
            rs_copy(t - LAG).wait_send()

        so, sa, ss = rem(t, 2), rem(t, A_SLOTS), rem(t, LAG)

        def body(rows):
            sendb[ss, rows, :] = own[so, 1 - x, rows, :] + ra[sa, 1 - x, rows, :]
            acc[ss, rows, :] = own[so, x, rows, :] + ra[sa, x, rows, :]

        row_loop(RB, body)
        rs_copy(t).start()

        @pl.when(t + 2 < MATS)
        def _():
            own_copy(t + 2).start()

        @pl.when(t + LEAD < MATS)
        def _():
            @pl.when(t + LEAD >= A_SLOTS)
            def _():
                a_copy(t + LEAD - A_SLOTS).wait_send()

            a_copy(t + LEAD).start()

    def finish(j):
        mom_load(j).wait()

        @pl.when(j >= 2)
        def _():
            mom_store(j - 2).wait()

        k = rem(j, DEVS)
        r = lax.div(j, DEVS)

        @pl.when((j >= DEVS) & (k != me))
        def _():
            u_copy(j - DEVS).wait_send()

        rs_copy(j).wait_recv()
        sm, ss, sr = rem(j, 2), rem(j, LAG), rem(j, B_SLOTS)

        def body(rows):
            mean = (acc[ss, rows, :] + recvb[sr, rows, :]) * 0.25
            new = MOMENTUM * momi[sm, rows, :] + mean
            momq[sm, rows, :] = new
            ust[k, rows, :] = (mean + MOMENTUM * new).astype(BF16)

        row_loop(RB, body)

        @pl.when(k != me)
        def _():
            u_copy(j).start()

        mom_store(j).start()

        @pl.when(j + 2 < MATS)
        def _():
            mom_load(j + 2).start()

        for half in range(2):
            @pl.when((k == me) & (y == half))
            def _():
                def put(rows):
                    dst = pl.ds(pl.multiple_of(dp * RB + rows.start, CHUNK), CHUNK)
                    xb[r, dst, half * CB:(half + 1) * CB] = ust[k, rows, :]

                row_loop(RB, put)

    def normalize(r):
        def square(i, total):
            v = xb[r, pl.ds(pl.multiple_of(i * CHUNK, CHUNK), CHUNK), :].astype(F32)
            return total + jnp.sum((v * v).reshape(CHUNK // 8, 8, COLS), axis=0)

        total = lax.fori_loop(0, ROWS // CHUNK, square, jnp.zeros((8, COLS), F32))
        norm = jnp.sqrt(jnp.sum(total, keepdims=True)) + NORM_EPS

        def scale(rows):
            xb[r, rows, :] = (xb[r, rows, :].astype(F32) / norm).astype(BF16)

        row_loop(ROWS, scale)

    def iterate(r):
        @pl.loop(0, COLS // 256)
        def _(m):
            cols = pl.ds(pl.multiple_of(m * 256, 256), 256)
            gram[cols, :] = lax.dot_general(
                xb[r, :, cols], xb[r], (((0,), (0,)), ((), ())), preferred_element_type=F32
            ).astype(BF16)

        @pl.loop(0, COLS // 256)
        def _(m):
            rows = pl.ds(pl.multiple_of(m * 256, 256), 256)
            part = gram[rows, :]
            square = jnp.dot(part, gram[...], preferred_element_type=F32)
            poly[rows, :] = (COEF_B * part.astype(F32) + COEF_C * square).astype(BF16)

        @pl.loop(0, ROWS // 512)
        def _(m):
            rows = pl.ds(pl.multiple_of(m * 512, 512), 512)
            part = xb[r, rows, :]
            prod = jnp.dot(part, poly[...], preferred_element_type=F32)
            xb[r, rows, :] = (COEF_A * part.astype(F32) + prod).astype(BF16)

    def ortho(r, s):
        @pl.when(s == 0)
        def _():
            @pl.loop(1, DEVS)
            def _(i):
                yy, dd = coords(i)
                remote(
                    ust.at[0], xblock(r, dd, yy), u_send.at[0],
                    u_recv.at[r * DEVS + yy * 4 + dd], partner,
                ).wait_recv()

            normalize(r)

        iterate(r)

        @pl.when(s == NS_STEPS - 1)
        def _():
            @pl.loop(0, DEVS)
            def _(n):
                i = rem(n + 4, DEVS)

                @pl.when(i != 0)
                def _():
                    x_copy(r, i).start()

            for half in range(2):
                @pl.when(y == half)
                def _():
                    def put(rows):
                        src = pl.ds(pl.multiple_of(dp * RB + rows.start, CHUNK), CHUNK)
                        rx[r * DEVS + me, rows, :] = xb[r, src, half * CB:(half + 1) * CB]

                    row_loop(RB, put)

    def forward(w):
        f_copy_in = remote(
            wst.at[0], wb_o.at[f_mat(w), nbr_dp], w_nbr.at[0], wx_recv.at[f_mat(w)], nbr
        )
        f_copy_in.wait_recv()
        f_copy(w).start()

    def weights(w):
        j = w_mat(w)

        @pl.when(rem(w, DEVS) != 0)
        def _():
            remote(xblock(0, 0, 0), rx.at[j], x_send.at[0], x_recv.at[j], nbr).wait_recv()

        wt_load(w).wait()

        @pl.when(w >= 2)
        def _():
            wt_store(w - 2).wait()

        @pl.when(w >= DEVS)
        def _():
            old = w_copies(w - DEVS)
            old[0].wait()
            old[1].wait_send()
            old[2].wait_send()

        s2, s8 = rem(w, 2), rem(w, DEVS)
        lr = rate[j]
        wd = decay[0]

        def body(rows):
            cur = wti[s2, rows, :]
            new = cur - lr * (OUT_SCALE * rx[j, rows, :].astype(F32) + wd * cur)
            wtq[s2, rows, :] = new
            wst[s8, rows, :] = new.astype(BF16)

        row_loop(RB, body)
        now = w_copies(w)
        now[2].start()
        now[1].start()
        now[0].start()
        wt_store(w).start()

        @pl.when(w + 2 < MATS)
        def _():
            wt_load(w + 2).start()

        @pl.when(w >= DEVS)
        def _():
            forward(w - DEVS)

    for t in range(2):
        own_copy(t).start()
    for t in range(2):
        mom_load(t).start()
        wt_load(t).start()

    barrier = pltpu.get_barrier_semaphore()
    for i in range(1, DEVS):
        yy, dd = coords(i)
        pl.semaphore_signal(barrier, inc=1, device_id={"tp": yy, "dp": dd}, device_id_type=MESH)
    pl.semaphore_wait(barrier, DEVS - 1)

    for t in range(LEAD):
        a_copy(t).start()

    def w_done(t):
        return (
            jnp.clip(2 * (t - W_START[0]), 0, 8)
            + jnp.clip(2 * (t - W_START[1]), 0, 8)
            + jnp.clip(8 * (t - W_START[2]), 0, 8)
        )

    @pl.loop(0, STEPS)
    def _(t):
        @pl.when((t >= LAG) & (t < MATS + LAG))
        def _():
            finish(t - LAG)

        @pl.when(t < MATS)
        def _():
            presum(t)

        pl.loop(w_done(t), w_done(t + 1))(weights)

        r = jnp.where(t >= NS_START[2], 2, jnp.where(t >= NS_START[1], 1, 0))
        base = jnp.where(
            t >= NS_START[2], NS_START[2], jnp.where(t >= NS_START[1], NS_START[1], NS_START[0])
        )

        @pl.when((t >= base) & (t < base + NS_STEPS))
        def _():
            ortho(r, t - base)

    @pl.loop(MATS - DEVS, MATS)
    def _(w):
        forward(w)

    for t in range(MATS - LAG, MATS):
        rs_copy(t).wait_send()
    for t in range(MATS - A_SLOTS, MATS):
        a_copy(t).wait_send()
    for j in range(MATS - 2, MATS):
        mom_store(j).wait()
        wt_store(j).wait()

    @pl.loop(MATS - DEVS, MATS)
    def _(j):
        @pl.when(rem(j, DEVS) != me)
        def _():
            u_copy(j).wait_send()

        old = w_copies(j)
        old[0].wait()
        old[1].wait_send()
        old[2].wait_send()

    @pl.loop(0, ROUNDS)
    def _(r):
        @pl.loop(1, DEVS)
        def _(i):
            x_copy(r, i).wait_send()

    @pl.loop(0, MATS)
    def _(w):
        j = w_mat(w)
        remote(wst.at[0], wb_o.at[j, dp], w_par.at[0], wp_recv.at[j], partner).wait_recv()
        f_copy(w).wait_send()
        ref = wb_o.at[j, 3 - dp]
        remote(ref, ref, f_send.at[j], f_recv.at[j], partner).wait_recv()


def solution(mesh):
    def local_step(grad_local, mom_local, weight_local, learn_rate, decay_rate):
        hbm = pl.BlockSpec(memory_space=pl.ANY)
        smem = pl.BlockSpec(memory_space=pltpu.SMEM)
        dma = pltpu.SemaphoreType.DMA
        block = (RB, CB)
        mom_new, weight_new, weight_full = pl.pallas_call(
            kernel,
            name="muon_step",
            out_shape=(
                jax.ShapeDtypeStruct((MATS,) + block, F32),
                jax.ShapeDtypeStruct((MATS,) + block, F32),
                jax.ShapeDtypeStruct((MATS, 4) + block, BF16),
            ),
            in_specs=[hbm, hbm, hbm, smem, smem],
            out_specs=[hbm, hbm, hbm],
            scratch_shapes=[
                pltpu.VMEM((2, 2) + block, F32),
                pltpu.VMEM((A_SLOTS, 2) + block, F32),
                pltpu.VMEM((LAG,) + block, F32),
                pltpu.VMEM((B_SLOTS,) + block, F32),
                pltpu.VMEM((LAG,) + block, F32),
                pltpu.VMEM((2,) + block, F32),
                pltpu.VMEM((2,) + block, F32),
                pltpu.VMEM((2,) + block, F32),
                pltpu.VMEM((2,) + block, F32),
                pltpu.VMEM((DEVS,) + block, BF16),
                pltpu.VMEM((DEVS,) + block, BF16),
                pltpu.VMEM((ROUNDS, ROWS, COLS), BF16),
                pltpu.VMEM((MATS,) + block, BF16),
                pltpu.VMEM((COLS, COLS), BF16),
                pltpu.VMEM((COLS, COLS), BF16),
                dma((2,)), dma((A_SLOTS,)), dma((A_SLOTS,)), dma((LAG,)), dma((B_SLOTS,)),
                dma((2,)), dma((2,)), dma((2,)), dma((2,)),
                dma((DEVS,)), dma((MATS,)), dma((MATS,)), dma((MATS,)),
                dma((DEVS,)), dma((DEVS,)), dma((DEVS,)), dma((MATS,)), dma((MATS,)),
                dma((MATS,)), dma((MATS,)),
            ],
            compiler_params=pltpu.CompilerParams(
                collective_id=0, has_side_effects=True, vmem_limit_bytes=67_000_000
            ),
            cost_estimate=pl.CostEstimate(
                flops=3 * 28_700_000_000, bytes_accessed=400_000_000, transcendentals=0
            ),
        )(
            grad_local.reshape((MATS, 2, 2) + block),
            mom_local,
            weight_local,
            learn_rate,
            decay_rate.reshape((1,)),
        )
        return mom_new, weight_new, weight_full.reshape(MATS, ROWS, CB)

    return jax.shard_map(
        local_step,
        mesh=mesh,
        in_specs=(P(("rep", "dp"), None, None, "tp"), P("rep", "dp", "tp"), P("rep", "dp", "tp"), P("rep"), P()),
        out_specs=(P("rep", "dp", "tp"), P("rep", "dp", "tp"), P("rep", None, "tp")),
        check_vma=False,
    )
```

```python
import math

import jax
import jax.numpy as jnp
from jax import lax
from jax.experimental import pallas as pl
from jax.experimental.pallas import tpu as pltpu
from jax.sharding import PartitionSpec as P


MOMENTUM = 0.95
NS_STEPS = 5
COEF_A = 3.4445
COEF_B = -4.7750
COEF_C = 2.0315
NORM_EPS = 1e-7

MESH = pl.DeviceIdType.MESH
F32 = jnp.float32
BF16 = jnp.bfloat16

MATS = 24
ROWS = 2048
COLS = 768
DEVS = 8
ROUNDS = MATS // DEVS
RB = ROWS // 4
CB = COLS // 2
OUT_SCALE = 0.2 * math.sqrt(max(ROWS, COLS))

LAG = 3
LEAD = 2
A_SLOTS = 2 * LEAD
B_SLOTS = 2 * LAG
NS_START = (8 + LAG + 2, 16 + LAG + 2, 24 + LAG)
W_START = (NS_START[0] + 7, NS_START[2], NS_START[2] + 5)
STEPS = NS_START[2] + 6
CHUNK = 64
HEAD = MATS - DEVS
TAIL_A = 6
TAIL_B = DEVS - TAIL_A


def rem(a, b):
    return lax.rem(a, b)


def row_loop(total, body):
    @pl.loop(0, total // CHUNK)
    def _(i):
        body(pl.ds(pl.multiple_of(i * CHUNK, CHUNK), CHUNK))


def kernel(
    grad, mom, wt, rate, decay,
    mom_o, wt_o, wb_o, tail_a, tail_b,
    own, ra, sendb, recvb, acc, momi, momq, wti, wtq, ust, wst, xb, rx, gram, poly,
    own_sem, a_send, a_recv, rs_send, rs_recv, momi_sem, momq_sem, wti_sem, wtq_sem,
    u_send, u_recv, x_send, x_recv, w_loc, w_par, w_nbr, wp_recv, wx_recv, f_send, f_recv,
):
    dp = lax.axis_index("dp")
    y = lax.axis_index("tp")
    x = lax.div(dp, 2)
    c = rem(dp, 2)
    me = y * 4 + dp
    partner = {"tp": y, "dp": x * 2 + (1 - c)}
    nbr_dp = (1 - x) * 2 + c
    nbr = {"tp": y, "dp": nbr_dp}

    def coords(i):
        dx, dy, dc = lax.div(i, 4), rem(lax.div(i, 2), 2), rem(i, 2)
        yy = rem(y + dy, 2)
        dd = rem(x + dx, 2) * 2 + rem(c + dc, 2)
        return yy, dd

    def remote(src, dst, ss, rs, dev):
        return pltpu.make_async_remote_copy(
            src_ref=src, dst_ref=dst, send_sem=ss, recv_sem=rs, device_id=dev, device_id_type=MESH
        )

    def xblock(r, dd, yy):
        return xb.at[
            r, pl.ds(pl.multiple_of(dd * RB, RB), RB), pl.ds(pl.multiple_of(yy * CB, CB), CB)
        ]

    def own_copy(t):
        s = rem(t, 2)
        return pltpu.make_async_copy(grad.at[t, :, c], own.at[s], own_sem.at[s])

    def a_copy(t):
        s = rem(t, A_SLOTS)
        return remote(grad.at[t, :, 1 - c], ra.at[s], a_send.at[s], a_recv.at[s], partner)

    def rs_copy(t):
        s, d = rem(t, LAG), rem(t, B_SLOTS)
        return remote(sendb.at[s], recvb.at[d], rs_send.at[s], rs_recv.at[d], nbr)

    def mom_load(j):
        s = rem(j, 2)
        return pltpu.make_async_copy(mom.at[j], momi.at[s], momi_sem.at[s])

    def mom_store(j):
        s = rem(j, 2)
        return pltpu.make_async_copy(momq.at[s], mom_o.at[j], momq_sem.at[s])

    def u_copy(j):
        k = rem(j, DEVS)
        r = lax.div(j, DEVS)
        dev = {"tp": lax.div(k, 4), "dp": rem(k, 4)}
        return remote(ust.at[k], xblock(r, dp, y), u_send.at[k], u_recv.at[r * DEVS + me], dev)

    def x_copy(r, i):
        yy, dd = coords(i)
        j = r * DEVS + me
        return remote(
            xblock(r, dd, yy), rx.at[j], x_send.at[r * DEVS + i], x_recv.at[j], {"tp": yy, "dp": dd}
        )

    def w_mat(w):
        yy, dd = coords(rem(w, DEVS))
        return lax.div(w, DEVS) * DEVS + yy * 4 + dd

    def wt_load(w):
        s = rem(w, 2)
        return pltpu.make_async_copy(wt.at[w_mat(w)], wti.at[s], wti_sem.at[s])

    def wt_store(w):
        s = rem(w, 2)
        return pltpu.make_async_copy(wtq.at[s], wt_o.at[w_mat(w)], wtq_sem.at[s])

    def w_copies(w):
        j, s = w_mat(w), rem(w, DEVS)
        dst = wb_o.at[j, dp]
        return (
            pltpu.make_async_copy(wst.at[s], dst, w_loc.at[s]),
            remote(wst.at[s], dst, w_par.at[s], wp_recv.at[j], partner),
            remote(wst.at[s], dst, w_nbr.at[s], wx_recv.at[j], nbr),
        )

    def tail_copy(w, part):
        j, s = w_mat(w) - HEAD, rem(w, DEVS)
        dst = tail_b.at[j - TAIL_A] if part else tail_a.at[j]
        return pltpu.make_async_copy(wst.at[s], dst, w_loc.at[s])

    def f_mat(w):
        i = rem(w, DEVS)
        dx, dy, dc = lax.div(i, 4), rem(lax.div(i, 2), 2), rem(i, 2)
        dd = rem(1 - x + dx, 2) * 2 + rem(c + dc, 2)
        return lax.div(w, DEVS) * DEVS + rem(y + dy, 2) * 4 + dd

    def f_copy(w):
        j = f_mat(w)
        ref = wb_o.at[j, nbr_dp]
        return remote(ref, ref, f_send.at[j], f_recv.at[j], partner)

    def presum(t):
        own_copy(t).wait()
        a_copy(t).wait_recv()

        @pl.when(t >= LAG)
        def _():
            rs_copy(t - LAG).wait_send()

        so, sa, ss = rem(t, 2), rem(t, A_SLOTS), rem(t, LAG)

        def body(rows):
            sendb[ss, rows, :] = own[so, 1 - x, rows, :] + ra[sa, 1 - x, rows, :]
            acc[ss, rows, :] = own[so, x, rows, :] + ra[sa, x, rows, :]

        row_loop(RB, body)
        rs_copy(t).start()

        @pl.when(t + 2 < MATS)
        def _():
            own_copy(t + 2).start()

        @pl.when(t + LEAD < MATS)
        def _():
            @pl.when(t + LEAD >= A_SLOTS)
            def _():
                a_copy(t + LEAD - A_SLOTS).wait_send()

            a_copy(t + LEAD).start()

    def finish(j):
        mom_load(j).wait()

        @pl.when(j >= 2)
        def _():
            mom_store(j - 2).wait()

        k = rem(j, DEVS)
        r = lax.div(j, DEVS)

        @pl.when((j >= DEVS) & (k != me))
        def _():
            u_copy(j - DEVS).wait_send()

        rs_copy(j).wait_recv()
        sm, ss, sr = rem(j, 2), rem(j, LAG), rem(j, B_SLOTS)

        def body(rows):
            mean = (acc[ss, rows, :] + recvb[sr, rows, :]) * 0.25
            new = MOMENTUM * momi[sm, rows, :] + mean
            momq[sm, rows, :] = new
            ust[k, rows, :] = (mean + MOMENTUM * new).astype(BF16)

        row_loop(RB, body)

        @pl.when(k != me)
        def _():
            u_copy(j).start()

        mom_store(j).start()

        @pl.when(j + 2 < MATS)
        def _():
            mom_load(j + 2).start()

        for half in range(2):
            @pl.when((k == me) & (y == half))
            def _():
                def put(rows):
                    dst = pl.ds(pl.multiple_of(dp * RB + rows.start, CHUNK), CHUNK)
                    xb[r, dst, half * CB:(half + 1) * CB] = ust[k, rows, :]

                row_loop(RB, put)

    def normalize(r):
        def square(i, total):
            v = xb[r, pl.ds(pl.multiple_of(i * CHUNK, CHUNK), CHUNK), :].astype(F32)
            return total + jnp.sum((v * v).reshape(CHUNK // 8, 8, COLS), axis=0)

        total = lax.fori_loop(0, ROWS // CHUNK, square, jnp.zeros((8, COLS), F32))
        norm = jnp.sqrt(jnp.sum(total, keepdims=True)) + NORM_EPS

        def scale(rows):
            xb[r, rows, :] = (xb[r, rows, :].astype(F32) / norm).astype(BF16)

        row_loop(ROWS, scale)

    def iterate(r):
        @pl.loop(0, COLS // 256)
        def _(m):
            cols = pl.ds(pl.multiple_of(m * 256, 256), 256)
            gram[cols, :] = lax.dot_general(
                xb[r, :, cols], xb[r], (((0,), (0,)), ((), ())), preferred_element_type=F32
            ).astype(BF16)

        @pl.loop(0, COLS // 256)
        def _(m):
            rows = pl.ds(pl.multiple_of(m * 256, 256), 256)
            part = gram[rows, :]
            square = jnp.dot(part, gram[...], preferred_element_type=F32)
            poly[rows, :] = (COEF_B * part.astype(F32) + COEF_C * square).astype(BF16)

        @pl.loop(0, ROWS // 512)
        def _(m):
            rows = pl.ds(pl.multiple_of(m * 512, 512), 512)
            part = xb[r, rows, :]
            prod = jnp.dot(part, poly[...], preferred_element_type=F32)
            xb[r, rows, :] = (COEF_A * part.astype(F32) + prod).astype(BF16)

    def ortho(r, s):
        @pl.when(s == 0)
        def _():
            @pl.loop(1, DEVS)
            def _(i):
                yy, dd = coords(i)
                remote(
                    ust.at[0], xblock(r, dd, yy), u_send.at[0],
                    u_recv.at[r * DEVS + yy * 4 + dd], partner,
                ).wait_recv()

            normalize(r)

        iterate(r)

        @pl.when(s == NS_STEPS - 1)
        def _():
            @pl.loop(0, DEVS)
            def _(n):
                i = rem(n + 4, DEVS)

                @pl.when(i != 0)
                def _():
                    x_copy(r, i).start()

            for half in range(2):
                @pl.when(y == half)
                def _():
                    def put(rows):
                        src = pl.ds(pl.multiple_of(dp * RB + rows.start, CHUNK), CHUNK)
                        rx[r * DEVS + me, rows, :] = xb[r, src, half * CB:(half + 1) * CB]

                    row_loop(RB, put)

    def forward(w):
        f_copy_in = remote(
            wst.at[0], wb_o.at[f_mat(w), nbr_dp], w_nbr.at[0], wx_recv.at[f_mat(w)], nbr
        )
        f_copy_in.wait_recv()
        f_copy(w).start()

    def weights(w):
        j = w_mat(w)

        @pl.when(rem(w, DEVS) != 0)
        def _():
            remote(xblock(0, 0, 0), rx.at[j], x_send.at[0], x_recv.at[j], nbr).wait_recv()

        wt_load(w).wait()

        @pl.when(w >= 2)
        def _():
            wt_store(w - 2).wait()

        @pl.when(w >= DEVS)
        def _():
            old = w_copies(w - DEVS)
            old[0].wait()
            old[1].wait_send()
            old[2].wait_send()

        s2, s8 = rem(w, 2), rem(w, DEVS)
        lr = rate[j]
        wd = decay[0]

        def body(rows):
            cur = wti[s2, rows, :]
            new = cur - lr * (OUT_SCALE * rx[j, rows, :].astype(F32) + wd * cur)
            wtq[s2, rows, :] = new
            wst[s8, rows, :] = new.astype(BF16)

        row_loop(RB, body)

        @pl.when(w < HEAD)
        def _():
            now = w_copies(w)
            now[2].start()
            now[1].start()
            now[0].start()

        @pl.when((w >= HEAD) & (j < HEAD + TAIL_A))
        def _():
            tail_copy(w, False).start()

        @pl.when((w >= HEAD) & (j >= HEAD + TAIL_A))
        def _():
            tail_copy(w, True).start()

        wt_store(w).start()

        @pl.when(w + 2 < MATS)
        def _():
            wt_load(w + 2).start()

        @pl.when(w >= DEVS)
        def _():
            forward(w - DEVS)

    for t in range(2):
        own_copy(t).start()
    for t in range(2):
        mom_load(t).start()
        wt_load(t).start()

    barrier = pltpu.get_barrier_semaphore()
    for i in range(1, DEVS):
        yy, dd = coords(i)
        pl.semaphore_signal(barrier, inc=1, device_id={"tp": yy, "dp": dd}, device_id_type=MESH)
    pl.semaphore_wait(barrier, DEVS - 1)

    for t in range(LEAD):
        a_copy(t).start()

    def w_done(t):
        return (
            jnp.clip(2 * (t - W_START[0]), 0, 8)
            + jnp.clip(2 * (t - W_START[1]), 0, 8)
            + jnp.clip(8 * (t - W_START[2]), 0, 8)
        )

    @pl.loop(0, STEPS)
    def _(t):
        @pl.when((t >= LAG) & (t < MATS + LAG))
        def _():
            finish(t - LAG)

        @pl.when(t < MATS)
        def _():
            presum(t)

        pl.loop(w_done(t), w_done(t + 1))(weights)

        r = jnp.where(t >= NS_START[2], 2, jnp.where(t >= NS_START[1], 1, 0))
        base = jnp.where(
            t >= NS_START[2], NS_START[2], jnp.where(t >= NS_START[1], NS_START[1], NS_START[0])
        )

        @pl.when((t >= base) & (t < base + NS_STEPS))
        def _():
            ortho(r, t - base)

    for t in range(MATS - LAG, MATS):
        rs_copy(t).wait_send()
    for t in range(MATS - A_SLOTS, MATS):
        a_copy(t).wait_send()
    for j in range(MATS - 2, MATS):
        mom_store(j).wait()
        wt_store(j).wait()

    @pl.loop(MATS - DEVS, MATS)
    def _(j):
        @pl.when(rem(j, DEVS) != me)
        def _():
            u_copy(j).wait_send()

        pltpu.make_async_copy(wst.at[0], tail_a.at[0], w_loc.at[rem(j, DEVS)]).wait()

    @pl.loop(0, ROUNDS)
    def _(r):
        @pl.loop(1, DEVS)
        def _(i):
            x_copy(r, i).wait_send()

    @pl.loop(0, HEAD)
    def _(w):
        j = w_mat(w)
        remote(wst.at[0], wb_o.at[j, dp], w_par.at[0], wp_recv.at[j], partner).wait_recv()
        f_copy(w).wait_send()
        ref = wb_o.at[j, 3 - dp]
        remote(ref, ref, f_send.at[j], f_recv.at[j], partner).wait_recv()


def publish_kernel(mom, wt, wb, mom_o, wt_o, wb_o):
    mom_o[...] = mom[...]
    wt_o[...] = wt[...]
    wb_o[...] = wb[...]


def publish(mom, wt, wb):
    steps = HEAD
    small = pl.BlockSpec((MATS * RB // steps, CB), lambda i: (i, 0))
    large = pl.BlockSpec((ROWS, CB), lambda i: (i, 0))
    return pl.pallas_call(
        publish_kernel,
        name="publish",
        grid=(steps,),
        out_shape=(
            jax.ShapeDtypeStruct((MATS * RB, CB), F32),
            jax.ShapeDtypeStruct((MATS * RB, CB), F32),
            jax.ShapeDtypeStruct((MATS * ROWS, CB), BF16),
        ),
        in_specs=[small, small, large],
        out_specs=[small, small, large],
        cost_estimate=pl.CostEstimate(
            flops=40_000_000_000, bytes_accessed=126_000_000, transcendentals=0
        ),
    )(mom.reshape(-1, CB), wt.reshape(-1, CB), wb.reshape(-1, CB))


def fill_kernel(own, par, nbr, fwd, whole, out):
    dp = lax.axis_index("dp")
    c = rem(dp, 2)
    out[0, dp] = own[0]
    out[0, dp + 1 - 2 * c] = par[0]
    out[0, rem(dp + 2, 4)] = nbr[0]
    out[0, 3 - dp] = fwd[0]


def fill(whole, first, own, par, nbr, fwd):
    count = own.shape[0]
    part = pl.BlockSpec((1, RB, CB), lambda i: (i, 0, 0))
    return pl.pallas_call(
        fill_kernel,
        name="fill",
        grid=(count,),
        out_shape=jax.ShapeDtypeStruct(whole.shape, whole.dtype),
        in_specs=[part] * 4 + [pl.BlockSpec(memory_space=pl.ANY)],
        out_specs=pl.BlockSpec((1, 4, RB, CB), lambda i: (i + first, 0, 0, 0)),
        input_output_aliases={4: 0},
        cost_estimate=pl.CostEstimate(
            flops=count * 1_000_000_000, bytes_accessed=count * 3_200_000, transcendentals=0
        ),
    )(own, par, nbr, fwd, whole)


def solution(mesh):
    def local_step(grad_local, mom_local, weight_local, learn_rate, decay_rate):
        hbm = pl.BlockSpec(memory_space=pl.ANY)
        smem = pl.BlockSpec(memory_space=pltpu.SMEM)
        dma = pltpu.SemaphoreType.DMA
        block = (RB, CB)
        mom_new, weight_new, head, tail_a, tail_b = pl.pallas_call(
            kernel,
            name="muon_step",
            out_shape=(
                jax.ShapeDtypeStruct((MATS,) + block, F32),
                jax.ShapeDtypeStruct((MATS,) + block, F32),
                jax.ShapeDtypeStruct((HEAD, 4) + block, BF16),
                jax.ShapeDtypeStruct((TAIL_A,) + block, BF16),
                jax.ShapeDtypeStruct((TAIL_B,) + block, BF16),
            ),
            in_specs=[hbm, hbm, hbm, smem, smem],
            out_specs=[hbm] * 5,
            scratch_shapes=[
                pltpu.VMEM((2, 2) + block, F32),
                pltpu.VMEM((A_SLOTS, 2) + block, F32),
                pltpu.VMEM((LAG,) + block, F32),
                pltpu.VMEM((B_SLOTS,) + block, F32),
                pltpu.VMEM((LAG,) + block, F32),
                pltpu.VMEM((2,) + block, F32),
                pltpu.VMEM((2,) + block, F32),
                pltpu.VMEM((2,) + block, F32),
                pltpu.VMEM((2,) + block, F32),
                pltpu.VMEM((DEVS,) + block, BF16),
                pltpu.VMEM((DEVS,) + block, BF16),
                pltpu.VMEM((ROUNDS, ROWS, COLS), BF16),
                pltpu.VMEM((MATS,) + block, BF16),
                pltpu.VMEM((COLS, COLS), BF16),
                pltpu.VMEM((COLS, COLS), BF16),
                dma((2,)), dma((A_SLOTS,)), dma((A_SLOTS,)), dma((LAG,)), dma((B_SLOTS,)),
                dma((2,)), dma((2,)), dma((2,)), dma((2,)),
                dma((DEVS,)), dma((MATS,)), dma((MATS,)), dma((MATS,)),
                dma((DEVS,)), dma((DEVS,)), dma((DEVS,)), dma((MATS,)), dma((MATS,)),
                dma((MATS,)), dma((MATS,)),
            ],
            compiler_params=pltpu.CompilerParams(
                collective_id=0, has_side_effects=True, vmem_limit_bytes=67_000_000
            ),
            cost_estimate=pl.CostEstimate(
                flops=3 * 28_700_000_000, bytes_accessed=400_000_000, transcendentals=0
            ),
        )(
            grad_local.reshape((MATS, 2, 2) + block),
            mom_local,
            weight_local,
            learn_rate,
            decay_rate.reshape((1,)),
        )
        across = [(0, 2), (1, 3), (2, 0), (3, 1)]
        beside = [(0, 1), (1, 0), (2, 3), (3, 2)]

        def move(value, pairs):
            return lax.ppermute(value, "dp", pairs)

        nbr_a = move(tail_a, across)
        nbr_b = move(tail_b, across)
        par_a = move(tail_a, beside)
        par_b = move(tail_b, beside)
        fwd_a = move(nbr_a, beside)
        fwd_b = move(nbr_b, beside)
        mom_new, weight_new, full = publish(mom_new, weight_new, head)
        full = full.reshape((MATS, 4) + block)
        full = fill(full, HEAD, tail_a, par_a, nbr_a, fwd_a)
        full = fill(full, HEAD + TAIL_A, tail_b, par_b, nbr_b, fwd_b)
        return (
            mom_new.reshape((MATS,) + block),
            weight_new.reshape((MATS,) + block),
            full.reshape(MATS, ROWS, CB),
        )

    return jax.shard_map(
        local_step,
        mesh=mesh,
        in_specs=(P(("rep", "dp"), None, None, "tp"), P("rep", "dp", "tp"), P("rep", "dp", "tp"), P("rep"), P()),
        out_specs=(P("rep", "dp", "tp"), P("rep", "dp", "tp"), P("rep", None, "tp")),
        check_vma=False,
    )
```

```python
import functools
import math

import jax
import jax.numpy as jnp
from jax import lax
from jax.experimental import pallas as pl
from jax.experimental.pallas import tpu as pltpu
from jax.sharding import PartitionSpec as P


MOMENTUM = 0.95
NS_STEPS = 5
COEF_A = 3.4445
COEF_B = -4.7750
COEF_C = 2.0315
NORM_EPS = 1e-7

MESH = pl.DeviceIdType.MESH
F32 = jnp.float32
BF16 = jnp.bfloat16

MATS = 24
ROWS = 2048
COLS = 768
DEVS = 8
ROUNDS = MATS // DEVS
RB = ROWS // 4
CB = COLS // 2
OUT_SCALE = 0.2 * math.sqrt(max(ROWS, COLS))

LAG = 3
LEAD = 2
A_SLOTS = 2 * LEAD
B_SLOTS = 2 * LAG
NS_START = (8 + LAG + 2, 16 + LAG + 2, 24 + LAG)
W_START = (NS_START[0] + 7, NS_START[2])
STEPS = NS_START[2] + NS_STEPS
CHUNK = 64
HEAD = MATS - DEVS
TAILS = (5, 2, 1)
PIECES = 4
PIECE = RB // PIECES


def rem(a, b):
    return lax.rem(a, b)


def row_loop(total, body):
    @pl.loop(0, total // CHUNK)
    def _(i):
        body(pl.ds(pl.multiple_of(i * CHUNK, CHUNK), CHUNK))


def kernel(
    grad, mom, wt, rate, decay,
    mom_o, wt_o, wb_o, tail_a, tail_b, tail_c,
    own, ra, sendb, recvb, acc, momi, momq, wti, wtq, ust, wst, xb, rx, gram, poly,
    p_send, p_recv, own_sem, a_send, a_recv, rs_send, rs_recv, momi_sem, momq_sem, wti_sem, wtq_sem,
    u_send, u_recv, x_send, x_recv, w_loc, w_par, w_nbr, wp_recv, wx_recv, f_send, f_recv,
):
    dp = lax.axis_index("dp")
    y = lax.axis_index("tp")
    x = lax.div(dp, 2)
    c = rem(dp, 2)
    me = y * 4 + dp
    partner = {"tp": y, "dp": x * 2 + (1 - c)}
    nbr_dp = (1 - x) * 2 + c
    nbr = {"tp": y, "dp": nbr_dp}

    def coords(i):
        dx, dy, dc = lax.div(i, 4), rem(lax.div(i, 2), 2), rem(i, 2)
        yy = rem(y + dy, 2)
        dd = rem(x + dx, 2) * 2 + rem(c + dc, 2)
        return yy, dd

    def remote(src, dst, ss, rs, dev):
        return pltpu.make_async_remote_copy(
            src_ref=src, dst_ref=dst, send_sem=ss, recv_sem=rs, device_id=dev, device_id_type=MESH
        )

    def xblock(r, dd, yy):
        return xb.at[
            r, pl.ds(pl.multiple_of(dd * RB, RB), RB), pl.ds(pl.multiple_of(yy * CB, CB), CB)
        ]

    def own_copy(t):
        s = rem(t, 2)
        return pltpu.make_async_copy(grad.at[t, :, c], own.at[s], own_sem.at[s])

    def a_copy(t):
        s = rem(t, A_SLOTS)
        return remote(grad.at[t, :, 1 - c], ra.at[s], a_send.at[s], a_recv.at[s], partner)

    def rs_copy(t):
        s, d = rem(t, LAG), rem(t, B_SLOTS)
        return remote(sendb.at[s], recvb.at[d], rs_send.at[s], rs_recv.at[d], nbr)

    def mom_load(j):
        s = rem(j, 2)
        return pltpu.make_async_copy(mom.at[j], momi.at[s], momi_sem.at[s])

    def mom_store(j):
        s = rem(j, 2)
        return pltpu.make_async_copy(momq.at[s], mom_o.at[j], momq_sem.at[s])

    def u_copy(j):
        k = rem(j, DEVS)
        r = lax.div(j, DEVS)
        dev = {"tp": lax.div(k, 4), "dp": rem(k, 4)}
        return remote(ust.at[k], xblock(r, dp, y), u_send.at[k], u_recv.at[r * DEVS + me], dev)

    def x_copy(r, i):
        yy, dd = coords(i)
        j = r * DEVS + me
        return remote(
            xblock(r, dd, yy), rx.at[j], x_send.at[r * DEVS + i], x_recv.at[j], {"tp": yy, "dp": dd}
        )

    def w_mat(w):
        yy, dd = coords(rem(w, DEVS))
        return lax.div(w, DEVS) * DEVS + yy * 4 + dd

    def wt_load(w):
        s = rem(w, 2)
        return pltpu.make_async_copy(wt.at[w_mat(w)], wti.at[s], wti_sem.at[s])

    def wt_store(w):
        s = rem(w, 2)
        return pltpu.make_async_copy(wtq.at[s], wt_o.at[w_mat(w)], wtq_sem.at[s])

    def w_copies(w):
        j, s = w_mat(w), rem(w, DEVS)
        dst = wb_o.at[j, dp]
        return (
            pltpu.make_async_copy(wst.at[s], dst, w_loc.at[s]),
            remote(wst.at[s], dst, w_par.at[s], wp_recv.at[j], partner),
            remote(wst.at[s], dst, w_nbr.at[s], wx_recv.at[j], nbr),
        )

    def tail_copies(w):
        s = rem(w, DEVS)
        first = HEAD
        for ref, count in zip((tail_a, tail_b, tail_c), TAILS):
            yield first, first + count, lambda j, ref=ref, first=first: pltpu.make_async_copy(
                wst.at[s], ref.at[j - first], w_loc.at[s]
            )
            first += count

    def f_mat(w):
        i = rem(w, DEVS)
        dx, dy, dc = lax.div(i, 4), rem(lax.div(i, 2), 2), rem(i, 2)
        dd = rem(1 - x + dx, 2) * 2 + rem(c + dc, 2)
        return lax.div(w, DEVS) * DEVS + rem(y + dy, 2) * 4 + dd

    def f_copy(w):
        j = f_mat(w)
        ref = wb_o.at[j, nbr_dp]
        return remote(ref, ref, f_send.at[j], f_recv.at[j], partner)

    def presum(t):
        own_copy(t).wait()
        a_copy(t).wait_recv()

        @pl.when(t >= LAG)
        def _():
            rs_copy(t - LAG).wait_send()

        so, sa, ss = rem(t, 2), rem(t, A_SLOTS), rem(t, LAG)

        def body(rows):
            sendb[ss, rows, :] = own[so, 1 - x, rows, :] + ra[sa, 1 - x, rows, :]
            acc[ss, rows, :] = own[so, x, rows, :] + ra[sa, x, rows, :]

        row_loop(RB, body)
        rs_copy(t).start()

        @pl.when(t + 2 < MATS)
        def _():
            own_copy(t + 2).start()

        @pl.when(t + LEAD < MATS)
        def _():
            @pl.when(t + LEAD > A_SLOTS)
            def _():
                a_copy(t + LEAD - A_SLOTS).wait_send()

            a_copy(t + LEAD).start()

    def piece_copy(q):
        rows = pl.ds(q * PIECE, PIECE)
        side = 1 - x
        if q == PIECES:
            rows, side = pl.ds(0, RB), x
        return remote(
            grad.at[0, side, 1 - c, rows, :], ra.at[0, side, rows, :], p_send.at[q], p_recv.at[q], partner
        )

    def presum_first():
        own_copy(0).wait()
        for q in range(PIECES):
            piece_copy(q).wait_recv()
            rows = pl.ds(q * PIECE, PIECE)
            sendb[0, rows, :] = own[0, 1 - x, rows, :] + ra[0, 1 - x, rows, :]
            remote(
                sendb.at[0, rows, :], recvb.at[0, rows, :], rs_send.at[0], rs_recv.at[0], nbr
            ).start()
        piece_copy(PIECES).wait_recv()

        def body(rows):
            acc[0, rows, :] = own[0, x, rows, :] + ra[0, x, rows, :]

        row_loop(RB, body)
        own_copy(2).start()
        a_copy(LEAD).start()

    def finish(j):
        mom_load(j).wait()

        @pl.when(j >= 2)
        def _():
            mom_store(j - 2).wait()

        k = rem(j, DEVS)
        r = lax.div(j, DEVS)

        @pl.when((j >= DEVS) & (k != me))
        def _():
            u_copy(j - DEVS).wait_send()

        rs_copy(j).wait_recv()
        sm, ss, sr = rem(j, 2), rem(j, LAG), rem(j, B_SLOTS)

        def body(rows):
            mean = (acc[ss, rows, :] + recvb[sr, rows, :]) * 0.25
            new = MOMENTUM * momi[sm, rows, :] + mean
            momq[sm, rows, :] = new
            ust[k, rows, :] = (mean + MOMENTUM * new).astype(BF16)

        row_loop(RB, body)

        @pl.when(k != me)
        def _():
            u_copy(j).start()

        mom_store(j).start()

        @pl.when(j + 2 < MATS)
        def _():
            mom_load(j + 2).start()

        for half in range(2):
            @pl.when((k == me) & (y == half))
            def _():
                def put(rows):
                    dst = pl.ds(pl.multiple_of(dp * RB + rows.start, CHUNK), CHUNK)
                    xb[r, dst, half * CB:(half + 1) * CB] = ust[k, rows, :]

                row_loop(RB, put)

    def normalize(r):
        def square(i, total):
            v = xb[r, pl.ds(pl.multiple_of(i * CHUNK, CHUNK), CHUNK), :].astype(F32)
            return total + jnp.sum((v * v).reshape(CHUNK // 8, 8, COLS), axis=0)

        total = lax.fori_loop(0, ROWS // CHUNK, square, jnp.zeros((8, COLS), F32))
        norm = jnp.sqrt(jnp.sum(total, keepdims=True)) + NORM_EPS

        def scale(rows):
            xb[r, rows, :] = (xb[r, rows, :].astype(F32) / norm).astype(BF16)

        row_loop(ROWS, scale)

    def iterate(r):
        @pl.loop(0, COLS // 256)
        def _(m):
            cols = pl.ds(pl.multiple_of(m * 256, 256), 256)
            gram[cols, :] = lax.dot_general(
                xb[r, :, cols], xb[r], (((0,), (0,)), ((), ())), preferred_element_type=F32
            ).astype(BF16)

        @pl.loop(0, COLS // 256)
        def _(m):
            rows = pl.ds(pl.multiple_of(m * 256, 256), 256)
            part = gram[rows, :]
            square = jnp.dot(part, gram[...], preferred_element_type=F32)
            poly[rows, :] = (COEF_B * part.astype(F32) + COEF_C * square).astype(BF16)

        @pl.loop(0, ROWS // 512)
        def _(m):
            rows = pl.ds(pl.multiple_of(m * 512, 512), 512)
            part = xb[r, rows, :]
            prod = jnp.dot(part, poly[...], preferred_element_type=F32)
            xb[r, rows, :] = (COEF_A * part.astype(F32) + prod).astype(BF16)

    def ortho(r, s):
        @pl.when(s == 0)
        def _():
            @pl.loop(1, DEVS)
            def _(i):
                yy, dd = coords(i)
                remote(
                    ust.at[0], xblock(r, dd, yy), u_send.at[0],
                    u_recv.at[r * DEVS + yy * 4 + dd], partner,
                ).wait_recv()

            normalize(r)

        iterate(r)

        @pl.when(s == NS_STEPS - 1)
        def _():
            @pl.loop(0, DEVS)
            def _(n):
                i = rem(n + 4, DEVS)

                @pl.when(i != 0)
                def _():
                    x_copy(r, i).start()

            for half in range(2):
                @pl.when(y == half)
                def _():
                    def put(rows):
                        src = pl.ds(pl.multiple_of(dp * RB + rows.start, CHUNK), CHUNK)
                        rx[r * DEVS + me, rows, :] = xb[r, src, half * CB:(half + 1) * CB]

                    row_loop(RB, put)

    def forward(w):
        f_copy_in = remote(
            wst.at[0], wb_o.at[f_mat(w), nbr_dp], w_nbr.at[0], wx_recv.at[f_mat(w)], nbr
        )
        f_copy_in.wait_recv()
        f_copy(w).start()

    def weights(w):
        j = w_mat(w)

        @pl.when(rem(w, DEVS) != 0)
        def _():
            remote(xblock(0, 0, 0), rx.at[j], x_send.at[0], x_recv.at[j], nbr).wait_recv()

        wt_load(w).wait()

        @pl.when(w >= 2)
        def _():
            wt_store(w - 2).wait()

        @pl.when(w >= DEVS)
        def _():
            old = w_copies(w - DEVS)
            old[0].wait()
            old[1].wait_send()
            old[2].wait_send()

        s2, s8 = rem(w, 2), rem(w, DEVS)
        lr = rate[j]
        wd = decay[0]

        def body(rows):
            cur = wti[s2, rows, :]
            new = cur - lr * (OUT_SCALE * rx[j, rows, :].astype(F32) + wd * cur)
            wtq[s2, rows, :] = new
            wst[s8, rows, :] = new.astype(BF16)

        row_loop(RB, body)

        @pl.when(w < HEAD)
        def _():
            now = w_copies(w)
            now[2].start()
            now[1].start()
            now[0].start()

        for low, high, copy in tail_copies(w):
            @pl.when((w >= HEAD) & (j >= low) & (j < high))
            def _():
                copy(j).start()

        wt_store(w).start()

        @pl.when(w + 2 < MATS)
        def _():
            wt_load(w + 2).start()

        @pl.when((w >= DEVS) & (w < HEAD))
        def _():
            forward(w - DEVS)

    for t in range(2):
        own_copy(t).start()
    for t in range(2):
        mom_load(t).start()
        wt_load(t).start()

    barrier = pltpu.get_barrier_semaphore()
    for i in range(1, DEVS):
        yy, dd = coords(i)
        pl.semaphore_signal(barrier, inc=1, device_id={"tp": yy, "dp": dd}, device_id_type=MESH)
    pl.semaphore_wait(barrier, DEVS - 1)

    for q in range(PIECES + 1):
        piece_copy(q).start()
    for t in range(1, LEAD):
        a_copy(t).start()
    presum_first()

    def w_done(t):
        return (
            jnp.clip(2 * (t - W_START[0]), 0, 8)
            + jnp.clip(2 * (t - W_START[1]), 0, 8)
        )

    @pl.loop(0, STEPS)
    def _(t):
        @pl.when((t >= LAG) & (t < MATS + LAG))
        def _():
            finish(t - LAG)

        @pl.when((t >= 1) & (t < MATS))
        def _():
            presum(t)

        pl.loop(w_done(t), w_done(t + 1))(weights)

        r = jnp.where(t >= NS_START[2], 2, jnp.where(t >= NS_START[1], 1, 0))
        base = jnp.where(
            t >= NS_START[2], NS_START[2], jnp.where(t >= NS_START[1], NS_START[1], NS_START[0])
        )

        @pl.when((t >= base) & (t < base + NS_STEPS))
        def _():
            ortho(r, t - base)

    @pl.loop(HEAD - DEVS, HEAD)
    def _(w):
        forward(w)

    for q in range(PIECES + 1):
        piece_copy(q).wait_send()
    for t in range(MATS - LAG, MATS):
        rs_copy(t).wait_send()
    for t in range(MATS - A_SLOTS, MATS):
        a_copy(t).wait_send()
    for j in range(MATS - 2, MATS):
        mom_store(j).wait()

    @pl.loop(HEAD, MATS)
    def _(j):
        @pl.when(rem(j, DEVS) != me)
        def _():
            u_copy(j).wait_send()

    def drain_x(r):
        @pl.loop(1, DEVS)
        def _(i):
            x_copy(r, i).wait_send()

    pl.loop(0, ROUNDS - 1)(drain_x)

    @pl.loop(0, HEAD)
    def _(w):
        j = w_mat(w)
        remote(wst.at[0], wb_o.at[j, dp], w_par.at[0], wp_recv.at[j], partner).wait_recv()
        f_copy(w).wait_send()
        ref = wb_o.at[j, 3 - dp]
        remote(ref, ref, f_send.at[j], f_recv.at[j], partner).wait_recv()

    pl.loop(HEAD, MATS)(weights)
    drain_x(ROUNDS - 1)
    for w in range(HEAD, MATS):
        pltpu.make_async_copy(wst.at[0], tail_a.at[0], w_loc.at[w % DEVS]).wait()
    for w in range(MATS - 2, MATS):
        wt_store(w).wait()


def publish_kernel(mom, wt, wb, mom_o, wt_o, wb_o):
    mom_o[...] = mom[...]
    wt_o[...] = wt[...]
    wb_o[...] = wb[...]


def publish(mom, wt, wb):
    steps = HEAD
    small = pl.BlockSpec((MATS * RB // steps, CB), lambda i: (i, 0))
    large = pl.BlockSpec((ROWS, CB), lambda i: (i, 0))
    return pl.pallas_call(
        publish_kernel,
        name="publish",
        grid=(steps,),
        out_shape=(
            jax.ShapeDtypeStruct((MATS * RB, CB), F32),
            jax.ShapeDtypeStruct((MATS * RB, CB), F32),
            jax.ShapeDtypeStruct((MATS * ROWS, CB), BF16),
        ),
        in_specs=[small, small, large],
        out_specs=[small, small, large],
        cost_estimate=pl.CostEstimate(
            flops=40_000_000_000, bytes_accessed=126_000_000, transcendentals=0
        ),
    )(mom.reshape(-1, CB), wt.reshape(-1, CB), wb.reshape(-1, CB))


def fill_kernel(first, own, par, nbr, fwd, whole, out, sems):
    dp = lax.axis_index("dp")
    places = (dp, dp + 1 - 2 * rem(dp, 2), rem(dp + 2, 4), 3 - dp)
    copies = [
        pltpu.make_async_copy(ref.at[i], out.at[first + i, place], sems.at[n, i])
        for n, (ref, place) in enumerate(zip((own, par, nbr, fwd), places))
        for i in range(own.shape[0])
    ]
    for copy in copies:
        copy.start()
    for copy in copies:
        copy.wait()


def fill(whole, first, own, par, nbr, fwd):
    count = own.shape[0]
    hbm = pl.BlockSpec(memory_space=pl.ANY)
    return pl.pallas_call(
        functools.partial(fill_kernel, first),
        name="fill",
        out_shape=jax.ShapeDtypeStruct(whole.shape, whole.dtype),
        in_specs=[pl.BlockSpec(memory_space=pltpu.VMEM)] * 4 + [hbm],
        out_specs=hbm,
        scratch_shapes=[pltpu.SemaphoreType.DMA((4, count))],
        input_output_aliases={4: 0},
        compiler_params=pltpu.CompilerParams(vmem_limit_bytes=10 << 20),
        cost_estimate=pl.CostEstimate(
            flops=count * 1_000_000_000, bytes_accessed=count * 3_200_000, transcendentals=0
        ),
    )(own, par, nbr, fwd, whole)


def solution(mesh):
    def local_step(grad_local, mom_local, weight_local, learn_rate, decay_rate):
        hbm = pl.BlockSpec(memory_space=pl.ANY)
        smem = pl.BlockSpec(memory_space=pltpu.SMEM)
        dma = pltpu.SemaphoreType.DMA
        block = (RB, CB)
        mom_new, weight_new, head, *tails = pl.pallas_call(
            kernel,
            name="muon_step",
            out_shape=(
                jax.ShapeDtypeStruct((MATS,) + block, F32),
                jax.ShapeDtypeStruct((MATS,) + block, F32),
                jax.ShapeDtypeStruct((HEAD, 4) + block, BF16),
            )
            + tuple(jax.ShapeDtypeStruct((n,) + block, BF16) for n in TAILS),
            in_specs=[hbm, hbm, hbm, smem, smem],
            out_specs=[hbm] * (3 + len(TAILS)),
            scratch_shapes=[
                pltpu.VMEM((2, 2) + block, F32),
                pltpu.VMEM((A_SLOTS, 2) + block, F32),
                pltpu.VMEM((LAG,) + block, F32),
                pltpu.VMEM((B_SLOTS,) + block, F32),
                pltpu.VMEM((LAG,) + block, F32),
                pltpu.VMEM((2,) + block, F32),
                pltpu.VMEM((2,) + block, F32),
                pltpu.VMEM((2,) + block, F32),
                pltpu.VMEM((2,) + block, F32),
                pltpu.VMEM((DEVS,) + block, BF16),
                pltpu.VMEM((DEVS,) + block, BF16),
                pltpu.VMEM((ROUNDS, ROWS, COLS), BF16),
                pltpu.VMEM((MATS,) + block, BF16),
                pltpu.VMEM((COLS, COLS), BF16),
                pltpu.VMEM((COLS, COLS), BF16),
                dma((PIECES + 1,)), dma((PIECES + 1,)),
                dma((2,)), dma((A_SLOTS,)), dma((A_SLOTS,)), dma((LAG,)), dma((B_SLOTS,)),
                dma((2,)), dma((2,)), dma((2,)), dma((2,)),
                dma((DEVS,)), dma((MATS,)), dma((MATS,)), dma((MATS,)),
                dma((DEVS,)), dma((DEVS,)), dma((DEVS,)), dma((MATS,)), dma((MATS,)),
                dma((MATS,)), dma((MATS,)),
            ],
            compiler_params=pltpu.CompilerParams(
                collective_id=0, has_side_effects=True, vmem_limit_bytes=67_000_000
            ),
            cost_estimate=pl.CostEstimate(
                flops=3 * 28_700_000_000, bytes_accessed=400_000_000, transcendentals=0
            ),
        )(
            grad_local.reshape((MATS, 2, 2) + block),
            mom_local,
            weight_local,
            learn_rate,
            decay_rate.reshape((1,)),
        )
        across = [(0, 2), (1, 3), (2, 0), (3, 1)]
        beside = [(0, 1), (1, 0), (2, 3), (3, 2)]

        def move(value, pairs):
            return lax.ppermute(value, "dp", pairs)

        nbr = [move(part, across) for part in tails]
        par = [move(part, beside) for part in tails]
        fwd = [move(part, beside) for part in nbr]
        mom_new, weight_new, full = publish(mom_new, weight_new, head)
        full = full.reshape((MATS, 4) + block)
        for n, part in enumerate(tails):
            full = fill(full, HEAD + sum(TAILS[:n]), part, par[n], nbr[n], fwd[n])
        return (
            mom_new.reshape((MATS,) + block),
            weight_new.reshape((MATS,) + block),
            full.reshape(MATS, ROWS, CB),
        )

    return jax.shard_map(
        local_step,
        mesh=mesh,
        in_specs=(P(("rep", "dp"), None, None, "tp"), P("rep", "dp", "tp"), P("rep", "dp", "tp"), P("rep"), P()),
        out_specs=(P("rep", "dp", "tp"), P("rep", "dp", "tp"), P("rep", None, "tp")),
        check_vma=False,
    )
```

```python
import functools
import math

import jax
import jax.numpy as jnp
from jax import lax
from jax.experimental import pallas as pl
from jax.experimental.pallas import tpu as pltpu
from jax.sharding import PartitionSpec as P


MOMENTUM = 0.95
NS_STEPS = 5
COEF_A = 3.4445
COEF_B = -4.7750
COEF_C = 2.0315
NORM_EPS = 1e-7

MESH = pl.DeviceIdType.MESH
F32 = jnp.float32
BF16 = jnp.bfloat16

MATS = 24
ROWS = 2048
COLS = 768
DEVS = 8
ROUNDS = MATS // DEVS
RB = ROWS // 4
CB = COLS // 2
OUT_SCALE = 0.2 * math.sqrt(max(ROWS, COLS))

LAG = 3
LEAD = 2
A_SLOTS = 2 * LEAD
B_SLOTS = 2 * LAG
NS_START = (8 + LAG + 2, 16 + LAG + 2, 24 + LAG)
W_START = (NS_START[0] + 7, NS_START[2])
STEPS = NS_START[2] + NS_STEPS
CHUNK = 64
HEAD = MATS - DEVS
TAILS = (1, 4, 2, 1)
PIECES = 4
PIECE = RB // PIECES


def rem(a, b):
    return lax.rem(a, b)


def owner_of(yy, dd):
    return yy * 4 + rem(dd, 2) * 2 + lax.div(dd, 2)


def shifted(yy, dd, i):
    dx, dy, dc = lax.div(i, 4), rem(lax.div(i, 2), 2), rem(i, 2)
    xx = rem(lax.div(dd, 2) + dx, 2)
    return rem(yy + dy, 2), xx * 2 + rem(rem(dd, 2) + dc, 2)


def row_loop(total, body):
    @pl.loop(0, total // CHUNK)
    def _(i):
        body(pl.ds(pl.multiple_of(i * CHUNK, CHUNK), CHUNK))


def kernel(
    grad, mom, wt, rate, decay,
    mom_o, wt_o, wb_o, tail_0, tail_1, tail_2, tail_3, mid,
    own, ra, sendb, recvb, acc, momi, momq, wti, wtq, ust, wst, xb, rx, gram, poly,
    mid_recv, p_send, p_recv, own_sem, a_send, a_recv, rs_send, rs_recv, momi_sem, momq_sem, wti_sem, wtq_sem,
    u_send, u_recv, x_send, x_recv, w_loc, w_par, w_nbr, wp_recv, wx_recv, f_send, f_recv,
):
    dp = lax.axis_index("dp")
    y = lax.axis_index("tp")
    x = lax.div(dp, 2)
    c = rem(dp, 2)
    me = owner_of(y, dp)
    partner = {"tp": y, "dp": x * 2 + (1 - c)}
    nbr_dp = (1 - x) * 2 + c
    nbr = {"tp": y, "dp": nbr_dp}

    def coords(i):
        return shifted(y, dp, i)

    def remote(src, dst, ss, rs, dev):
        return pltpu.make_async_remote_copy(
            src_ref=src, dst_ref=dst, send_sem=ss, recv_sem=rs, device_id=dev, device_id_type=MESH
        )

    def xblock(r, dd, yy):
        return xb.at[
            r, pl.ds(pl.multiple_of(dd * RB, RB), RB), pl.ds(pl.multiple_of(yy * CB, CB), CB)
        ]

    def own_copy(t):
        s = rem(t, 2)
        return pltpu.make_async_copy(grad.at[t, :, c], own.at[s], own_sem.at[s])

    def a_copy(t):
        s = rem(t, A_SLOTS)
        return remote(grad.at[t, :, 1 - c], ra.at[s], a_send.at[s], a_recv.at[s], partner)

    def rs_copy(t):
        s, d = rem(t, LAG), rem(t, B_SLOTS)
        return remote(sendb.at[s], recvb.at[d], rs_send.at[s], rs_recv.at[d], nbr)

    def mom_load(j):
        s = rem(j, 2)
        return pltpu.make_async_copy(mom.at[j], momi.at[s], momi_sem.at[s])

    def mom_store(j):
        s = rem(j, 2)
        return pltpu.make_async_copy(momq.at[s], mom_o.at[j], momq_sem.at[s])

    def u_copy(j):
        k = rem(j, DEVS)
        r = lax.div(j, DEVS)
        dev = {"tp": lax.div(k, 4), "dp": rem(k, 2) * 2 + rem(lax.div(k, 2), 2)}
        return remote(ust.at[k], xblock(r, dp, y), u_send.at[k], u_recv.at[r * DEVS + me], dev)

    def x_copy(r, i):
        yy, dd = coords(i)
        j = r * DEVS + me
        return remote(
            xblock(r, dd, yy), rx.at[j], x_send.at[r * DEVS + i], x_recv.at[j], {"tp": yy, "dp": dd}
        )

    def w_mat(w):
        return lax.div(w, DEVS) * DEVS + owner_of(*coords(rem(w, DEVS)))

    def wt_load(w):
        s = rem(w, 2)
        return pltpu.make_async_copy(wt.at[w_mat(w)], wti.at[s], wti_sem.at[s])

    def wt_store(w):
        s = rem(w, 2)
        return pltpu.make_async_copy(wtq.at[s], wt_o.at[w_mat(w)], wtq_sem.at[s])

    def w_copies(w):
        j, s = w_mat(w), rem(w, DEVS)
        dst = wb_o.at[j, dp]
        return (
            pltpu.make_async_copy(wst.at[s], dst, w_loc.at[s]),
            remote(wst.at[s], dst, w_par.at[s], wp_recv.at[j], partner),
            remote(wst.at[s], dst, w_nbr.at[s], wx_recv.at[j], nbr),
        )

    def tail_copies(w):
        s = rem(w, DEVS)
        first = HEAD
        for ref, count in zip((tail_0, tail_1, tail_2, tail_3), TAILS):
            yield first, first + count, lambda ref=ref, first=first: pltpu.make_async_copy(
                wst.at[s], ref.at[w - first], w_loc.at[s]
            )
            first += count

    def mid_copy():
        return remote(wst.at[0], mid.at[0], w_nbr.at[0], mid_recv.at[0], nbr)

    def f_mat(w):
        return lax.div(w, DEVS) * DEVS + owner_of(*shifted(y, nbr_dp, rem(w, DEVS)))

    def f_copy(w):
        j = f_mat(w)
        ref = wb_o.at[j, nbr_dp]
        return remote(ref, ref, f_send.at[j], f_recv.at[j], partner)

    def presum(t):
        own_copy(t).wait()
        a_copy(t).wait_recv()

        @pl.when(t >= LAG)
        def _():
            rs_copy(t - LAG).wait_send()

        so, sa, ss = rem(t, 2), rem(t, A_SLOTS), rem(t, LAG)

        def body(rows):
            sendb[ss, rows, :] = own[so, 1 - x, rows, :] + ra[sa, 1 - x, rows, :]
            acc[ss, rows, :] = own[so, x, rows, :] + ra[sa, x, rows, :]

        row_loop(RB, body)
        rs_copy(t).start()

        @pl.when(t + 2 < MATS)
        def _():
            own_copy(t + 2).start()

        @pl.when(t + LEAD < MATS)
        def _():
            @pl.when(t + LEAD > A_SLOTS)
            def _():
                a_copy(t + LEAD - A_SLOTS).wait_send()

            a_copy(t + LEAD).start()

    def piece_copy(q):
        rows = pl.ds(q * PIECE, PIECE)
        side = 1 - x
        if q == PIECES:
            rows, side = pl.ds(0, RB), x
        return remote(
            grad.at[0, side, 1 - c, rows, :], ra.at[0, side, rows, :], p_send.at[q], p_recv.at[q], partner
        )

    def presum_first():
        own_copy(0).wait()
        for q in range(PIECES):
            piece_copy(q).wait_recv()
            rows = pl.ds(q * PIECE, PIECE)
            sendb[0, rows, :] = own[0, 1 - x, rows, :] + ra[0, 1 - x, rows, :]
            remote(
                sendb.at[0, rows, :], recvb.at[0, rows, :], rs_send.at[0], rs_recv.at[0], nbr
            ).start()
        piece_copy(PIECES).wait_recv()

        def body(rows):
            acc[0, rows, :] = own[0, x, rows, :] + ra[0, x, rows, :]

        row_loop(RB, body)
        own_copy(2).start()
        a_copy(LEAD).start()

    def finish(j):
        mom_load(j).wait()

        @pl.when(j >= 2)
        def _():
            mom_store(j - 2).wait()

        k = rem(j, DEVS)
        r = lax.div(j, DEVS)

        @pl.when((j >= DEVS) & (k != me))
        def _():
            u_copy(j - DEVS).wait_send()

        rs_copy(j).wait_recv()
        sm, ss, sr = rem(j, 2), rem(j, LAG), rem(j, B_SLOTS)

        def body(rows):
            mean = (acc[ss, rows, :] + recvb[sr, rows, :]) * 0.25
            new = MOMENTUM * momi[sm, rows, :] + mean
            momq[sm, rows, :] = new
            ust[k, rows, :] = (mean + MOMENTUM * new).astype(BF16)

        row_loop(RB, body)

        @pl.when(k != me)
        def _():
            u_copy(j).start()

        mom_store(j).start()

        @pl.when(j + 2 < MATS)
        def _():
            mom_load(j + 2).start()

        for half in range(2):
            @pl.when((k == me) & (y == half))
            def _():
                def put(rows):
                    dst = pl.ds(pl.multiple_of(dp * RB + rows.start, CHUNK), CHUNK)
                    xb[r, dst, half * CB:(half + 1) * CB] = ust[k, rows, :]

                row_loop(RB, put)

    def normalize(r):
        def square(i, total):
            v = xb[r, pl.ds(pl.multiple_of(i * CHUNK, CHUNK), CHUNK), :].astype(F32)
            return total + jnp.sum((v * v).reshape(CHUNK // 8, 8, COLS), axis=0)

        total = lax.fori_loop(0, ROWS // CHUNK, square, jnp.zeros((8, COLS), F32))
        norm = jnp.sqrt(jnp.sum(total, keepdims=True)) + NORM_EPS

        def scale(rows):
            xb[r, rows, :] = (xb[r, rows, :].astype(F32) / norm).astype(BF16)

        row_loop(ROWS, scale)

    def iterate(r):
        @pl.loop(0, COLS // 256)
        def _(m):
            cols = pl.ds(pl.multiple_of(m * 256, 256), 256)
            gram[cols, :] = lax.dot_general(
                xb[r, :, cols], xb[r], (((0,), (0,)), ((), ())), preferred_element_type=F32
            ).astype(BF16)

        @pl.loop(0, COLS // 256)
        def _(m):
            rows = pl.ds(pl.multiple_of(m * 256, 256), 256)
            part = gram[rows, :]
            square = jnp.dot(part, gram[...], preferred_element_type=F32)
            poly[rows, :] = (COEF_B * part.astype(F32) + COEF_C * square).astype(BF16)

        @pl.loop(0, ROWS // 512)
        def _(m):
            rows = pl.ds(pl.multiple_of(m * 512, 512), 512)
            part = xb[r, rows, :]
            prod = jnp.dot(part, poly[...], preferred_element_type=F32)
            xb[r, rows, :] = (COEF_A * part.astype(F32) + prod).astype(BF16)

    def ortho(r, s):
        @pl.when(s == 0)
        def _():
            @pl.loop(1, DEVS)
            def _(i):
                yy, dd = coords(i)
                remote(
                    ust.at[0], xblock(r, dd, yy), u_send.at[0],
                    u_recv.at[r * DEVS + owner_of(yy, dd)], partner,
                ).wait_recv()

            normalize(r)

        iterate(r)

        @pl.when(s == NS_STEPS - 1)
        def _():
            @pl.loop(0, DEVS)
            def _(n):
                i = rem(n + 4, DEVS)

                @pl.when(i != 0)
                def _():
                    x_copy(r, i).start()

            for half in range(2):
                @pl.when(y == half)
                def _():
                    def put(rows):
                        src = pl.ds(pl.multiple_of(dp * RB + rows.start, CHUNK), CHUNK)
                        rx[r * DEVS + me, rows, :] = xb[r, src, half * CB:(half + 1) * CB]

                    row_loop(RB, put)

    def forward(w):
        f_copy_in = remote(
            wst.at[0], wb_o.at[f_mat(w), nbr_dp], w_nbr.at[0], wx_recv.at[f_mat(w)], nbr
        )
        f_copy_in.wait_recv()
        f_copy(w).start()

    def weights(w):
        j = w_mat(w)

        @pl.when(rem(w, DEVS) != 0)
        def _():
            remote(xblock(0, 0, 0), rx.at[j], x_send.at[0], x_recv.at[j], nbr).wait_recv()

        wt_load(w).wait()

        @pl.when(w >= 2)
        def _():
            wt_store(w - 2).wait()

        @pl.when(w >= DEVS)
        def _():
            old = w_copies(w - DEVS)
            old[0].wait()
            old[1].wait_send()
            old[2].wait_send()

        s2, s8 = rem(w, 2), rem(w, DEVS)
        lr = rate[j]
        wd = decay[0]

        def body(rows):
            cur = wti[s2, rows, :]
            new = cur - lr * (OUT_SCALE * rx[j, rows, :].astype(F32) + wd * cur)
            wtq[s2, rows, :] = new
            wst[s8, rows, :] = new.astype(BF16)

        row_loop(RB, body)

        @pl.when(w < HEAD)
        def _():
            now = w_copies(w)
            now[2].start()
            now[1].start()
            now[0].start()

        for low, high, copy in tail_copies(w):
            @pl.when((w >= low) & (w < high))
            def _():
                copy().start()

        @pl.when(w == HEAD)
        def _():
            mid_copy().start()

        wt_store(w).start()

        @pl.when(w + 2 < MATS)
        def _():
            wt_load(w + 2).start()

        @pl.when((w >= DEVS) & (w < HEAD))
        def _():
            forward(w - DEVS)

    for t in range(2):
        own_copy(t).start()
    for t in range(2):
        mom_load(t).start()
        wt_load(t).start()

    barrier = pltpu.get_barrier_semaphore()
    for i in range(1, DEVS):
        yy, dd = coords(i)
        pl.semaphore_signal(barrier, inc=1, device_id={"tp": yy, "dp": dd}, device_id_type=MESH)
    pl.semaphore_wait(barrier, DEVS - 1)

    for q in range(PIECES + 1):
        piece_copy(q).start()
    for t in range(1, LEAD):
        a_copy(t).start()
    presum_first()

    def w_done(t):
        return (
            jnp.minimum(4 * jnp.clip(t - W_START[0], 0, 1) + 2 * jnp.clip(t - W_START[0] - 1, 0, 2), 8)
            + jnp.minimum(4 * jnp.clip(t - W_START[1], 0, 1) + 2 * jnp.clip(t - W_START[1] - 1, 0, 2), 8)
        )

    @pl.loop(0, STEPS)
    def _(t):
        @pl.when((t >= LAG) & (t < MATS + LAG))
        def _():
            finish(t - LAG)

        @pl.when((t >= 1) & (t < MATS))
        def _():
            presum(t)

        pl.loop(w_done(t), w_done(t + 1))(weights)

        r = jnp.where(t >= NS_START[2], 2, jnp.where(t >= NS_START[1], 1, 0))
        base = jnp.where(
            t >= NS_START[2], NS_START[2], jnp.where(t >= NS_START[1], NS_START[1], NS_START[0])
        )

        @pl.when((t >= base) & (t < base + NS_STEPS))
        def _():
            ortho(r, t - base)

    @pl.loop(HEAD - DEVS, HEAD)
    def _(w):
        forward(w)

    for q in range(PIECES + 1):
        piece_copy(q).wait_send()
    for t in range(MATS - LAG, MATS):
        rs_copy(t).wait_send()
    for t in range(MATS - A_SLOTS, MATS):
        a_copy(t).wait_send()
    for j in range(MATS - 2, MATS):
        mom_store(j).wait()

    @pl.loop(HEAD, MATS)
    def _(j):
        @pl.when(rem(j, DEVS) != me)
        def _():
            u_copy(j).wait_send()

    def drain_x(r):
        @pl.loop(1, DEVS)
        def _(i):
            x_copy(r, i).wait_send()

    pl.loop(0, ROUNDS - 1)(drain_x)

    @pl.loop(0, HEAD)
    def _(w):
        j = w_mat(w)
        remote(wst.at[0], wb_o.at[j, dp], w_par.at[0], wp_recv.at[j], partner).wait_recv()
        f_copy(w).wait_send()
        ref = wb_o.at[j, 3 - dp]
        remote(ref, ref, f_send.at[j], f_recv.at[j], partner).wait_recv()

    pl.loop(HEAD, MATS)(weights)
    drain_x(ROUNDS - 1)
    for w in range(HEAD, MATS):
        pltpu.make_async_copy(wst.at[0], tail_0.at[0], w_loc.at[w % DEVS]).wait()
    for w in range(MATS - 2, MATS):
        wt_store(w).wait()
    mid_copy().wait()


def publish_kernel(mom, wt, wb, mom_o, wt_o, wb_o):
    mom_o[...] = mom[...]
    wt_o[...] = wt[...]
    wb_o[...] = wb[...]


def publish(mom, wt, wb):
    steps = HEAD
    small = pl.BlockSpec((MATS * RB // steps, CB), lambda i: (i, 0))
    large = pl.BlockSpec((ROWS, CB), lambda i: (i, 0))
    return pl.pallas_call(
        publish_kernel,
        name="publish",
        grid=(steps,),
        out_shape=(
            jax.ShapeDtypeStruct((MATS * RB, CB), F32),
            jax.ShapeDtypeStruct((MATS * RB, CB), F32),
            jax.ShapeDtypeStruct((MATS * ROWS, CB), BF16),
        ),
        in_specs=[small, small, large],
        out_specs=[small, small, large],
        cost_estimate=pl.CostEstimate(
            flops=40_000_000_000, bytes_accessed=126_000_000, transcendentals=0
        ),
    )(mom.reshape(-1, CB), wt.reshape(-1, CB), wb.reshape(-1, CB))


def fill_kernel(first, own, par, nbr, fwd, whole, out, sems):
    dp = lax.axis_index("dp")
    y = lax.axis_index("tp")
    places = (dp, dp + 1 - 2 * rem(dp, 2), rem(dp + 2, 4), 3 - dp)
    copies = [
        pltpu.make_async_copy(
            ref.at[i], out.at[HEAD + owner_of(*shifted(y, place, first + i)), place], sems.at[n, i]
        )
        for n, (ref, place) in enumerate(zip((own, par, nbr, fwd), places))
        for i in range(own.shape[0])
    ]
    for copy in copies:
        copy.start()
    for copy in copies:
        copy.wait()


def fill(whole, first, own, par, nbr, fwd):
    count = own.shape[0]
    hbm = pl.BlockSpec(memory_space=pl.ANY)
    return pl.pallas_call(
        functools.partial(fill_kernel, first),
        name="fill",
        out_shape=jax.ShapeDtypeStruct(whole.shape, whole.dtype),
        in_specs=[pl.BlockSpec(memory_space=pltpu.VMEM)] * 4 + [hbm],
        out_specs=hbm,
        scratch_shapes=[pltpu.SemaphoreType.DMA((4, count))],
        input_output_aliases={4: 0},
        compiler_params=pltpu.CompilerParams(vmem_limit_bytes=10 << 20),
        cost_estimate=pl.CostEstimate(
            flops=count * 1_000_000_000, bytes_accessed=count * 3_200_000, transcendentals=0
        ),
    )(own, par, nbr, fwd, whole)


def solution(mesh):
    def local_step(grad_local, mom_local, weight_local, learn_rate, decay_rate):
        hbm = pl.BlockSpec(memory_space=pl.ANY)
        smem = pl.BlockSpec(memory_space=pltpu.SMEM)
        dma = pltpu.SemaphoreType.DMA
        block = (RB, CB)
        mom_new, weight_new, head, *tails, mid = pl.pallas_call(
            kernel,
            name="muon_step",
            out_shape=(
                jax.ShapeDtypeStruct((MATS,) + block, F32),
                jax.ShapeDtypeStruct((MATS,) + block, F32),
                jax.ShapeDtypeStruct((HEAD, 4) + block, BF16),
            )
            + tuple(jax.ShapeDtypeStruct((n,) + block, BF16) for n in TAILS + (1,)),
            in_specs=[hbm, hbm, hbm, smem, smem],
            out_specs=[hbm] * (4 + len(TAILS)),
            scratch_shapes=[
                pltpu.VMEM((2, 2) + block, F32),
                pltpu.VMEM((A_SLOTS, 2) + block, F32),
                pltpu.VMEM((LAG,) + block, F32),
                pltpu.VMEM((B_SLOTS,) + block, F32),
                pltpu.VMEM((LAG,) + block, F32),
                pltpu.VMEM((2,) + block, F32),
                pltpu.VMEM((2,) + block, F32),
                pltpu.VMEM((2,) + block, F32),
                pltpu.VMEM((2,) + block, F32),
                pltpu.VMEM((DEVS,) + block, BF16),
                pltpu.VMEM((DEVS,) + block, BF16),
                pltpu.VMEM((ROUNDS, ROWS, COLS), BF16),
                pltpu.VMEM((MATS,) + block, BF16),
                pltpu.VMEM((COLS, COLS), BF16),
                pltpu.VMEM((COLS, COLS), BF16),
                dma((1,)), dma((PIECES + 1,)), dma((PIECES + 1,)),
                dma((2,)), dma((A_SLOTS,)), dma((A_SLOTS,)), dma((LAG,)), dma((B_SLOTS,)),
                dma((2,)), dma((2,)), dma((2,)), dma((2,)),
                dma((DEVS,)), dma((MATS,)), dma((MATS,)), dma((MATS,)),
                dma((DEVS,)), dma((DEVS,)), dma((DEVS,)), dma((MATS,)), dma((MATS,)),
                dma((MATS,)), dma((MATS,)),
            ],
            compiler_params=pltpu.CompilerParams(
                collective_id=0, has_side_effects=True, vmem_limit_bytes=67_000_000
            ),
            cost_estimate=pl.CostEstimate(
                flops=3 * 28_700_000_000, bytes_accessed=400_000_000, transcendentals=0
            ),
        )(
            grad_local.reshape((MATS, 2, 2) + block),
            mom_local,
            weight_local,
            learn_rate,
            decay_rate.reshape((1,)),
        )
        across = [(0, 2), (1, 3), (2, 0), (3, 1)]
        beside = [(0, 1), (1, 0), (2, 3), (3, 2)]

        def move(value, pairs):
            return lax.ppermute(value, "dp", pairs)

        nbr = [mid] + [move(tails[n], across) for n in range(1, len(tails))]
        par = [move(part, beside) for part in tails]
        fwd = [move(part, beside) for part in nbr]
        mom_new, weight_new, full = publish(mom_new, weight_new, head)
        full = full.reshape((MATS, 4) + block)
        for n, part in enumerate(tails):
            full = fill(full, sum(TAILS[:n]), part, par[n], nbr[n], fwd[n])
        return (
            mom_new.reshape((MATS,) + block),
            weight_new.reshape((MATS,) + block),
            full.reshape(MATS, ROWS, CB),
        )

    return jax.shard_map(
        local_step,
        mesh=mesh,
        in_specs=(P(("rep", "dp"), None, None, "tp"), P("rep", "dp", "tp"), P("rep", "dp", "tp"), P("rep"), P()),
        out_specs=(P("rep", "dp", "tp"), P("rep", "dp", "tp"), P("rep", None, "tp")),
        check_vma=False,
    )
```

```python
import functools
import math

import jax
import jax.numpy as jnp
from jax import lax
from jax.experimental import pallas as pl
from jax.experimental.pallas import tpu as pltpu
from jax.sharding import PartitionSpec as P


MOMENTUM = 0.95
NS_STEPS = 5
COEF_A = 3.4445
COEF_B = -4.7750
COEF_C = 2.0315
NORM_EPS = 1e-7

MESH = pl.DeviceIdType.MESH
F32 = jnp.float32
BF16 = jnp.bfloat16

MATS = 24
ROWS = 2048
COLS = 768
DEVS = 8
ROUNDS = MATS // DEVS
RB = ROWS // 4
CB = COLS // 2
OUT_SCALE = 0.2 * math.sqrt(max(ROWS, COLS))

LAG = 3
LEAD = 2
A_SLOTS = 2 * LEAD
B_SLOTS = 2 * LAG
NS_START = (8 + LAG + 2, 16 + LAG + 2, 24 + LAG)
W_START = (NS_START[0] + 7, NS_START[2])
STEPS = NS_START[2] + NS_STEPS
CHUNK = 64
HEAD = MATS - DEVS
TAILS = (1, 4, 2, 1)
PIECES = 4
PIECE = RB // PIECES


def rem(a, b):
    return lax.rem(a, b)


def owner_of(yy, dd):
    return yy * 4 + rem(dd, 2) * 2 + lax.div(dd, 2)


def shifted(yy, dd, i):
    dx, dy, dc = lax.div(i, 4), rem(lax.div(i, 2), 2), rem(i, 2)
    xx = rem(lax.div(dd, 2) + dx, 2)
    return rem(yy + dy, 2), xx * 2 + rem(rem(dd, 2) + dc, 2)


def row_loop(total, body):
    @pl.loop(0, total // CHUNK)
    def _(i):
        body(pl.ds(pl.multiple_of(i * CHUNK, CHUNK), CHUNK))


def kernel(
    grad, mom, wt, rate, decay,
    mom_o, wt_o, wb_o, tail_0, tail_1, tail_2, tail_3, mid,
    own, ra, sendb, recvb, acc, momi, momq, wti, wtq, ust, wst, xb, rx, gram, poly,
    mid_recv, p_send, p_recv, own_sem, a_send, a_recv, rs_send, rs_recv, momi_sem, momq_sem, wti_sem, wtq_sem,
    u_send, u_recv, x_send, x_recv, w_loc, w_par, w_nbr, wp_recv, wx_recv, f_send, f_recv,
):
    dp = lax.axis_index("dp")
    y = lax.axis_index("tp")
    x = lax.div(dp, 2)
    c = rem(dp, 2)
    me = owner_of(y, dp)
    partner = {"tp": y, "dp": x * 2 + (1 - c)}
    nbr_dp = (1 - x) * 2 + c
    nbr = {"tp": y, "dp": nbr_dp}

    def coords(i):
        return shifted(y, dp, i)

    def remote(src, dst, ss, rs, dev):
        return pltpu.make_async_remote_copy(
            src_ref=src, dst_ref=dst, send_sem=ss, recv_sem=rs, device_id=dev, device_id_type=MESH
        )

    def xblock(r, dd, yy):
        return xb.at[
            r, pl.ds(pl.multiple_of(dd * RB, RB), RB), pl.ds(pl.multiple_of(yy * CB, CB), CB)
        ]

    def own_copy(t):
        s = rem(t, 2)
        return pltpu.make_async_copy(grad.at[t, :, c], own.at[s], own_sem.at[s])

    def a_copy(t):
        s = rem(t, A_SLOTS)
        return remote(grad.at[t, :, 1 - c], ra.at[s], a_send.at[s], a_recv.at[s], partner)

    def rs_copy(t):
        s, d = rem(t, LAG), rem(t, B_SLOTS)
        return remote(sendb.at[s], recvb.at[d], rs_send.at[s], rs_recv.at[d], nbr)

    def mom_load(j):
        s = rem(j, 2)
        return pltpu.make_async_copy(mom.at[j], momi.at[s], momi_sem.at[s])

    def mom_store(j):
        s = rem(j, 2)
        return pltpu.make_async_copy(momq.at[s], mom_o.at[j], momq_sem.at[s])

    def u_copy(j):
        k = rem(j, DEVS)
        r = lax.div(j, DEVS)
        dev = {"tp": lax.div(k, 4), "dp": rem(k, 2) * 2 + rem(lax.div(k, 2), 2)}
        return remote(ust.at[k], xblock(r, dp, y), u_send.at[k], u_recv.at[r * DEVS + me], dev)

    def x_copy(r, i):
        yy, dd = coords(i)
        j = r * DEVS + me
        return remote(
            xblock(r, dd, yy), rx.at[j], x_send.at[r * DEVS + i], x_recv.at[j], {"tp": yy, "dp": dd}
        )

    def w_mat(w):
        return lax.div(w, DEVS) * DEVS + owner_of(*coords(rem(w, DEVS)))

    def wt_load(w):
        s = rem(w, 2)
        return pltpu.make_async_copy(wt.at[w_mat(w)], wti.at[s], wti_sem.at[s])

    def wt_store(w):
        s = rem(w, 2)
        return pltpu.make_async_copy(wtq.at[s], wt_o.at[w_mat(w)], wtq_sem.at[s])

    def w_copies(w):
        j, s = w_mat(w), rem(w, DEVS)
        dst = wb_o.at[j, dp]
        return (
            pltpu.make_async_copy(wst.at[s], dst, w_loc.at[s]),
            remote(wst.at[s], dst, w_par.at[s], wp_recv.at[j], partner),
            remote(wst.at[s], dst, w_nbr.at[s], wx_recv.at[j], nbr),
        )

    def tail_copies(w):
        s = rem(w, DEVS)
        first = HEAD
        for ref, count in zip((tail_0, tail_1, tail_2, tail_3), TAILS):
            yield first, first + count, lambda ref=ref, first=first: pltpu.make_async_copy(
                wst.at[s], ref.at[w - first], w_loc.at[s]
            )
            first += count

    def mid_copy():
        return remote(wst.at[0], mid.at[0], w_nbr.at[0], mid_recv.at[0], nbr)

    def f_mat(w):
        return lax.div(w, DEVS) * DEVS + owner_of(*shifted(y, nbr_dp, rem(w, DEVS)))

    def f_copy(w):
        j = f_mat(w)
        ref = wb_o.at[j, nbr_dp]
        return remote(ref, ref, f_send.at[j], f_recv.at[j], partner)

    def presum(t):
        own_copy(t).wait()
        a_copy(t).wait_recv()

        @pl.when(t >= LAG)
        def _():
            rs_copy(t - LAG).wait_send()

        so, sa, ss = rem(t, 2), rem(t, A_SLOTS), rem(t, LAG)

        def body(rows):
            sendb[ss, rows, :] = own[so, 1 - x, rows, :] + ra[sa, 1 - x, rows, :]
            acc[ss, rows, :] = own[so, x, rows, :] + ra[sa, x, rows, :]

        row_loop(RB, body)
        rs_copy(t).start()

        @pl.when(t + 2 < MATS)
        def _():
            own_copy(t + 2).start()

        @pl.when(t + LEAD < MATS)
        def _():
            @pl.when(t + LEAD > A_SLOTS)
            def _():
                a_copy(t + LEAD - A_SLOTS).wait_send()

            a_copy(t + LEAD).start()

    def piece_copy(q):
        if q == PIECES:
            src, dst = grad.at[0, x, 1 - c], ra.at[0, x]
        else:
            rows = pl.ds(q * PIECE, PIECE)
            src, dst = wtq.at[0, rows, :], ra.at[0, 1 - x, rows, :]
        return remote(src, dst, p_send.at[q], p_recv.at[q], partner)

    def stage_copy():
        return pltpu.make_async_copy(grad.at[0, 1 - x, 1 - c], wtq.at[0], wtq_sem.at[0])

    def presum_first():
        own_copy(0).wait()
        for q in range(PIECES):
            piece_copy(q).wait_recv()
            rows = pl.ds(q * PIECE, PIECE)
            sendb[0, rows, :] = own[0, 1 - x, rows, :] + ra[0, 1 - x, rows, :]
            remote(
                sendb.at[0, rows, :], recvb.at[0, rows, :], rs_send.at[0], rs_recv.at[0], nbr
            ).start()
        piece_copy(PIECES).wait_recv()

        def body(rows):
            acc[0, rows, :] = own[0, x, rows, :] + ra[0, x, rows, :]

        row_loop(RB, body)
        own_copy(2).start()
        a_copy(LEAD).start()
        for q in range(PIECES + 1):
            piece_copy(q).wait_send()

    def finish(j):
        mom_load(j).wait()

        @pl.when(j >= 2)
        def _():
            mom_store(j - 2).wait()

        k = rem(j, DEVS)
        r = lax.div(j, DEVS)

        @pl.when((j >= DEVS) & (k != me))
        def _():
            u_copy(j - DEVS).wait_send()

        rs_copy(j).wait_recv()
        sm, ss, sr = rem(j, 2), rem(j, LAG), rem(j, B_SLOTS)

        def body(rows):
            mean = (acc[ss, rows, :] + recvb[sr, rows, :]) * 0.25
            new = MOMENTUM * momi[sm, rows, :] + mean
            momq[sm, rows, :] = new
            ust[k, rows, :] = (mean + MOMENTUM * new).astype(BF16)

        row_loop(RB, body)

        @pl.when(k != me)
        def _():
            u_copy(j).start()

        mom_store(j).start()

        @pl.when(j + 2 < MATS)
        def _():
            mom_load(j + 2).start()

        for half in range(2):
            @pl.when((k == me) & (y == half))
            def _():
                def put(rows):
                    dst = pl.ds(pl.multiple_of(dp * RB + rows.start, CHUNK), CHUNK)
                    xb[r, dst, half * CB:(half + 1) * CB] = ust[k, rows, :]

                row_loop(RB, put)

    def normalize(r):
        def square(i, total):
            v = xb[r, pl.ds(pl.multiple_of(i * CHUNK, CHUNK), CHUNK), :].astype(F32)
            return total + jnp.sum((v * v).reshape(CHUNK // 8, 8, COLS), axis=0)

        total = lax.fori_loop(0, ROWS // CHUNK, square, jnp.zeros((8, COLS), F32))
        norm = jnp.sqrt(jnp.sum(total, keepdims=True)) + NORM_EPS

        def scale(rows):
            xb[r, rows, :] = (xb[r, rows, :].astype(F32) / norm).astype(BF16)

        row_loop(ROWS, scale)

    def iterate(r):
        @pl.loop(0, COLS // 256)
        def _(m):
            cols = pl.ds(pl.multiple_of(m * 256, 256), 256)
            gram[cols, :] = lax.dot_general(
                xb[r, :, cols], xb[r], (((0,), (0,)), ((), ())), preferred_element_type=F32
            ).astype(BF16)

        @pl.loop(0, COLS // 256)
        def _(m):
            rows = pl.ds(pl.multiple_of(m * 256, 256), 256)
            part = gram[rows, :]
            square = jnp.dot(part, gram[...], preferred_element_type=F32)
            poly[rows, :] = (COEF_B * part.astype(F32) + COEF_C * square).astype(BF16)

        @pl.loop(0, ROWS // 512)
        def _(m):
            rows = pl.ds(pl.multiple_of(m * 512, 512), 512)
            part = xb[r, rows, :]
            prod = jnp.dot(part, poly[...], preferred_element_type=F32)
            xb[r, rows, :] = (COEF_A * part.astype(F32) + prod).astype(BF16)

    def ortho(r, s):
        @pl.when(s == 0)
        def _():
            @pl.loop(1, DEVS)
            def _(i):
                yy, dd = coords(i)
                remote(
                    ust.at[0], xblock(r, dd, yy), u_send.at[0],
                    u_recv.at[r * DEVS + owner_of(yy, dd)], partner,
                ).wait_recv()

            normalize(r)

        iterate(r)

        @pl.when(s == NS_STEPS - 1)
        def _():
            @pl.loop(0, DEVS)
            def _(n):
                i = rem(n + 4, DEVS)

                @pl.when(i != 0)
                def _():
                    x_copy(r, i).start()

            for half in range(2):
                @pl.when(y == half)
                def _():
                    def put(rows):
                        src = pl.ds(pl.multiple_of(dp * RB + rows.start, CHUNK), CHUNK)
                        rx[r * DEVS + me, rows, :] = xb[r, src, half * CB:(half + 1) * CB]

                    row_loop(RB, put)

    def forward(w):
        f_copy_in = remote(
            wst.at[0], wb_o.at[f_mat(w), nbr_dp], w_nbr.at[0], wx_recv.at[f_mat(w)], nbr
        )
        f_copy_in.wait_recv()
        f_copy(w).start()

    def weights(w):
        j = w_mat(w)

        @pl.when(rem(w, DEVS) != 0)
        def _():
            remote(xblock(0, 0, 0), rx.at[j], x_send.at[0], x_recv.at[j], nbr).wait_recv()

        wt_load(w).wait()

        @pl.when(w >= 2)
        def _():
            wt_store(w - 2).wait()

        @pl.when(w >= DEVS)
        def _():
            old = w_copies(w - DEVS)
            old[0].wait()
            old[1].wait_send()
            old[2].wait_send()

        s2, s8 = rem(w, 2), rem(w, DEVS)
        lr = rate[j]
        wd = decay[...]

        def body(rows):
            cur = wti[s2, rows, :]
            new = cur - lr * (OUT_SCALE * rx[j, rows, :].astype(F32) + wd * cur)
            wtq[s2, rows, :] = new
            wst[s8, rows, :] = new.astype(BF16)

        row_loop(RB, body)

        @pl.when(w < HEAD)
        def _():
            now = w_copies(w)
            now[2].start()
            now[1].start()
            now[0].start()

        for low, high, copy in tail_copies(w):
            @pl.when((w >= low) & (w < high))
            def _():
                copy().start()

        @pl.when(w == HEAD)
        def _():
            mid_copy().start()

        wt_store(w).start()

        @pl.when(w + 2 < MATS)
        def _():
            wt_load(w + 2).start()

        @pl.when((w >= DEVS) & (w < HEAD))
        def _():
            forward(w - DEVS)

    stage_copy().start()
    for t in range(2):
        own_copy(t).start()
    for t in range(2):
        mom_load(t).start()
        wt_load(t).start()

    barrier = pltpu.get_barrier_semaphore()
    for i in range(1, DEVS):
        yy, dd = coords(i)
        pl.semaphore_signal(barrier, inc=1, device_id={"tp": yy, "dp": dd}, device_id_type=MESH)
    pl.semaphore_wait(barrier, DEVS - 1)

    stage_copy().wait()
    for q in range(PIECES + 1):
        piece_copy(q).start()
    for t in range(1, LEAD):
        a_copy(t).start()
    presum_first()

    def w_done(t):
        return (
            jnp.minimum(4 * jnp.clip(t - W_START[0], 0, 1) + 2 * jnp.clip(t - W_START[0] - 1, 0, 2), 8)
            + jnp.minimum(4 * jnp.clip(t - W_START[1], 0, 1) + 2 * jnp.clip(t - W_START[1] - 1, 0, 2), 8)
        )

    @pl.loop(0, STEPS)
    def _(t):
        @pl.when((t >= LAG) & (t < MATS + LAG))
        def _():
            finish(t - LAG)

        @pl.when((t >= 1) & (t < MATS))
        def _():
            presum(t)

        pl.loop(w_done(t), w_done(t + 1))(weights)

        r = jnp.where(t >= NS_START[2], 2, jnp.where(t >= NS_START[1], 1, 0))
        base = jnp.where(
            t >= NS_START[2], NS_START[2], jnp.where(t >= NS_START[1], NS_START[1], NS_START[0])
        )

        @pl.when((t >= base) & (t < base + NS_STEPS))
        def _():
            ortho(r, t - base)

    @pl.loop(HEAD - DEVS, HEAD)
    def _(w):
        forward(w)

    for t in range(MATS - LAG, MATS):
        rs_copy(t).wait_send()
    for t in range(MATS - A_SLOTS, MATS):
        a_copy(t).wait_send()
    for j in range(MATS - 2, MATS):
        mom_store(j).wait()

    @pl.loop(HEAD, MATS)
    def _(j):
        @pl.when(rem(j, DEVS) != me)
        def _():
            u_copy(j).wait_send()

    def drain_x(r):
        @pl.loop(1, DEVS)
        def _(i):
            x_copy(r, i).wait_send()

    pl.loop(0, ROUNDS - 1)(drain_x)

    @pl.loop(0, HEAD)
    def _(w):
        j = w_mat(w)
        remote(wst.at[0], wb_o.at[j, dp], w_par.at[0], wp_recv.at[j], partner).wait_recv()
        f_copy(w).wait_send()
        ref = wb_o.at[j, 3 - dp]
        remote(ref, ref, f_send.at[j], f_recv.at[j], partner).wait_recv()

    pl.loop(HEAD, MATS)(weights)
    drain_x(ROUNDS - 1)
    for w in range(HEAD, MATS):
        pltpu.make_async_copy(wst.at[0], tail_0.at[0], w_loc.at[w % DEVS]).wait()
    for w in range(MATS - 2, MATS):
        wt_store(w).wait()
    mid_copy().wait()


def publish_kernel(mom, wt, wb, mom_o, wt_o, wb_o):
    mom_o[...] = mom[...]
    wt_o[...] = wt[...]
    wb_o[...] = wb[...]


def publish(mom, wt, wb):
    steps = HEAD
    small = pl.BlockSpec((MATS * RB // steps, CB), lambda i: (i, 0))
    large = pl.BlockSpec((ROWS, CB), lambda i: (i, 0))
    return pl.pallas_call(
        publish_kernel,
        name="publish",
        grid=(steps,),
        out_shape=(
            jax.ShapeDtypeStruct((MATS * RB, CB), F32),
            jax.ShapeDtypeStruct((MATS * RB, CB), F32),
            jax.ShapeDtypeStruct((MATS * ROWS, CB), BF16),
        ),
        in_specs=[small, small, large],
        out_specs=[small, small, large],
        cost_estimate=pl.CostEstimate(
            flops=40_000_000_000, bytes_accessed=126_000_000, transcendentals=0
        ),
        compiler_params=pltpu.CompilerParams(vmem_limit_bytes=44 << 20),
    )(mom.reshape(-1, CB), wt.reshape(-1, CB), wb.reshape(-1, CB))


def fill_kernel(first, own, par, nbr, fwd, whole, out, sems):
    dp = lax.axis_index("dp")
    y = lax.axis_index("tp")
    places = (dp, dp + 1 - 2 * rem(dp, 2), rem(dp + 2, 4), 3 - dp)
    copies = [
        pltpu.make_async_copy(
            ref.at[i], out.at[HEAD + owner_of(*shifted(y, place, first + i)), place], sems.at[n, i]
        )
        for n, (ref, place) in enumerate(zip((own, par, nbr, fwd), places))
        for i in range(own.shape[0])
    ]
    for copy in copies:
        copy.start()
    for copy in copies:
        copy.wait()


def fill(whole, first, own, par, nbr, fwd):
    count = own.shape[0]
    hbm = pl.BlockSpec(memory_space=pl.ANY)
    return pl.pallas_call(
        functools.partial(fill_kernel, first),
        name="fill",
        out_shape=jax.ShapeDtypeStruct(whole.shape, whole.dtype),
        in_specs=[pl.BlockSpec(memory_space=pltpu.VMEM)] * 4 + [hbm],
        out_specs=hbm,
        scratch_shapes=[pltpu.SemaphoreType.DMA((4, count))],
        input_output_aliases={4: 0},
        compiler_params=pltpu.CompilerParams(vmem_limit_bytes=10 << 20),
        cost_estimate=pl.CostEstimate(
            flops=count * 1_000_000_000, bytes_accessed=count * 3_200_000, transcendentals=0
        ),
    )(own, par, nbr, fwd, whole)


def solution(mesh):
    def local_step(grad_local, mom_local, weight_local, learn_rate, decay_rate):
        hbm = pl.BlockSpec(memory_space=pl.ANY)
        smem = pl.BlockSpec(memory_space=pltpu.SMEM)
        dma = pltpu.SemaphoreType.DMA
        block = (RB, CB)
        mom_new, weight_new, head, *tails, mid = pl.pallas_call(
            kernel,
            name="muon_step",
            out_shape=(
                jax.ShapeDtypeStruct((MATS,) + block, F32),
                jax.ShapeDtypeStruct((MATS,) + block, F32),
                jax.ShapeDtypeStruct((HEAD, 4) + block, BF16),
            )
            + tuple(jax.ShapeDtypeStruct((n,) + block, BF16) for n in TAILS + (1,)),
            in_specs=[hbm, hbm, hbm, smem, smem],
            out_specs=[hbm] * (4 + len(TAILS)),
            scratch_shapes=[
                pltpu.VMEM((2, 2) + block, F32),
                pltpu.VMEM((A_SLOTS, 2) + block, F32),
                pltpu.VMEM((LAG,) + block, F32),
                pltpu.VMEM((B_SLOTS,) + block, F32),
                pltpu.VMEM((LAG,) + block, F32),
                pltpu.VMEM((2,) + block, F32),
                pltpu.VMEM((2,) + block, F32),
                pltpu.VMEM((2,) + block, F32),
                pltpu.VMEM((2,) + block, F32),
                pltpu.VMEM((DEVS,) + block, BF16),
                pltpu.VMEM((DEVS,) + block, BF16),
                pltpu.VMEM((ROUNDS, ROWS, COLS), BF16),
                pltpu.VMEM((MATS,) + block, BF16),
                pltpu.VMEM((COLS, COLS), BF16),
                pltpu.VMEM((COLS, COLS), BF16),
                dma((1,)), dma((PIECES + 1,)), dma((PIECES + 1,)),
                dma((2,)), dma((A_SLOTS,)), dma((A_SLOTS,)), dma((LAG,)), dma((B_SLOTS,)),
                dma((2,)), dma((2,)), dma((2,)), dma((2,)),
                dma((DEVS,)), dma((MATS,)), dma((MATS,)), dma((MATS,)),
                dma((DEVS,)), dma((DEVS,)), dma((DEVS,)), dma((MATS,)), dma((MATS,)),
                dma((MATS,)), dma((MATS,)),
            ],
            compiler_params=pltpu.CompilerParams(
                collective_id=0, has_side_effects=True, vmem_limit_bytes=67_000_000
            ),
            cost_estimate=pl.CostEstimate(
                flops=3 * 28_700_000_000, bytes_accessed=400_000_000, transcendentals=0
            ),
        )(
            grad_local.reshape((MATS, 2, 2) + block),
            mom_local,
            weight_local,
            learn_rate,
            decay_rate,
        )
        across = [(0, 2), (1, 3), (2, 0), (3, 1)]
        beside = [(0, 1), (1, 0), (2, 3), (3, 2)]

        def move(value, pairs):
            return lax.ppermute(value, "dp", pairs)

        nbr = [mid] + [move(tails[n], across) for n in range(1, len(tails))]
        par = [move(part, beside) for part in tails]
        fwd = [move(part, beside) for part in nbr]
        mom_new, weight_new, full = publish(mom_new, weight_new, head)
        full = full.reshape((MATS, 4) + block)
        for n, part in enumerate(tails):
            full = fill(full, sum(TAILS[:n]), part, par[n], nbr[n], fwd[n])
        return (
            mom_new.reshape((MATS,) + block),
            weight_new.reshape((MATS,) + block),
            full.reshape(MATS, ROWS, CB),
        )

    return jax.shard_map(
        local_step,
        mesh=mesh,
        in_specs=(P(("rep", "dp"), None, None, "tp"), P("rep", "dp", "tp"), P("rep", "dp", "tp"), P("rep"), P()),
        out_specs=(P("rep", "dp", "tp"), P("rep", "dp", "tp"), P("rep", None, "tp")),
        check_vma=False,
    )
```

```python
import functools
import math

import jax
import jax.numpy as jnp
from jax import lax
from jax.experimental import pallas as pl
from jax.experimental.pallas import tpu as pltpu
from jax.sharding import PartitionSpec as P


MOMENTUM = 0.95
NS_STEPS = 5
COEF_A = 3.4445
COEF_B = -4.7750
COEF_C = 2.0315
NORM_EPS = 1e-7

MESH = pl.DeviceIdType.MESH
F32 = jnp.float32
BF16 = jnp.bfloat16

MATS = 24
ROWS = 2048
COLS = 768
DEVS = 8
ROUNDS = MATS // DEVS
RB = ROWS // 4
CB = COLS // 2
OUT_SCALE = 0.2 * math.sqrt(max(ROWS, COLS))

LAG = 3
LEAD = 2
A_SLOTS = 2 * LEAD
B_SLOTS = 2 * LAG
NS_START = (8 + LAG + 2, 16 + LAG + 2, 24 + LAG)
W_START = (NS_START[0] + 7, NS_START[2])
STEPS = NS_START[2] + NS_STEPS
CHUNK = 64
HEAD = MATS - DEVS
TAILS = ((0, 1, 0, RB), (1, 4, 0, RB), (5, 2, 0, RB), (7, 1, 0, RB // 2), (7, 1, RB // 2, RB // 2))
PIECES = 4
PIECE = RB // PIECES


def rem(a, b):
    return lax.rem(a, b)


def owner_of(yy, dd):
    return yy * 4 + rem(dd, 2) * 2 + lax.div(dd, 2)


def shifted(yy, dd, i):
    dx, dy, dc = lax.div(i, 4), rem(lax.div(i, 2), 2), rem(i, 2)
    xx = rem(lax.div(dd, 2) + dx, 2)
    return rem(yy + dy, 2), xx * 2 + rem(rem(dd, 2) + dc, 2)


def row_loop(total, body):
    @pl.loop(0, total // CHUNK)
    def _(i):
        body(pl.ds(pl.multiple_of(i * CHUNK, CHUNK), CHUNK))


def kernel(
    grad, mom, wt, rate_in, decay,
    mom_o, wt_o, wb_o, tail_0, tail_1, tail_2, tail_3, tail_4, mid,
    rate, rate_sem, own, ra, sendb, recvb, acc, momi, momq, wti, wtq, ust, wst, xb, rx, gram, poly,
    mid_recv, p_send, p_recv, own_sem, a_send, a_recv, rs_send, rs_recv, momi_sem, momq_sem, wti_sem, wtq_sem,
    u_send, u_recv, x_send, x_recv, w_loc, w_par, w_nbr, wp_recv, wx_recv, f_send, f_recv,
):
    dp = lax.axis_index("dp")
    y = lax.axis_index("tp")
    x = lax.div(dp, 2)
    c = rem(dp, 2)
    me = owner_of(y, dp)
    partner = {"tp": y, "dp": x * 2 + (1 - c)}
    nbr_dp = (1 - x) * 2 + c
    nbr = {"tp": y, "dp": nbr_dp}

    def coords(i):
        return shifted(y, dp, i)

    def remote(src, dst, ss, rs, dev):
        return pltpu.make_async_remote_copy(
            src_ref=src, dst_ref=dst, send_sem=ss, recv_sem=rs, device_id=dev, device_id_type=MESH
        )

    def xblock(r, dd, yy):
        return xb.at[
            r, pl.ds(pl.multiple_of(dd * RB, RB), RB), pl.ds(pl.multiple_of(yy * CB, CB), CB)
        ]

    def rate_copy():
        return pltpu.make_async_copy(rate_in, rate, rate_sem.at[0])

    def own_copy(t):
        s = rem(t, 2)
        return pltpu.make_async_copy(grad.at[t, :, c], own.at[s], own_sem.at[s])

    def a_copy(t):
        s = rem(t, A_SLOTS)
        return remote(grad.at[t, :, 1 - c], ra.at[s], a_send.at[s], a_recv.at[s], partner)

    def rs_copy(t):
        s, d = rem(t, LAG), rem(t, B_SLOTS)
        return remote(sendb.at[s], recvb.at[d], rs_send.at[s], rs_recv.at[d], nbr)

    def mom_load(j):
        s = rem(j, 2)
        return pltpu.make_async_copy(mom.at[j], momi.at[s], momi_sem.at[s])

    def mom_store(j):
        s = rem(j, 2)
        return pltpu.make_async_copy(momq.at[s], mom_o.at[j], momq_sem.at[s])

    def u_copy(j):
        k = rem(j, DEVS)
        r = lax.div(j, DEVS)
        dev = {"tp": lax.div(k, 4), "dp": rem(k, 2) * 2 + rem(lax.div(k, 2), 2)}
        return remote(ust.at[k], xblock(r, dp, y), u_send.at[k], u_recv.at[r * DEVS + me], dev)

    def x_copy(r, i):
        yy, dd = coords(i)
        j = r * DEVS + me
        return remote(
            xblock(r, dd, yy), rx.at[j], x_send.at[r * DEVS + i], x_recv.at[j], {"tp": yy, "dp": dd}
        )

    def w_mat(w):
        return lax.div(w, DEVS) * DEVS + owner_of(*coords(rem(w, DEVS)))

    def wt_load(w):
        s = rem(w, 2)
        return pltpu.make_async_copy(wt.at[w_mat(w)], wti.at[s], wti_sem.at[s])

    def wt_store(w):
        s = rem(w, 2)
        return pltpu.make_async_copy(wtq.at[s], wt_o.at[w_mat(w)], wtq_sem.at[s])

    def w_copies(w):
        j, s = w_mat(w), rem(w, DEVS)
        dst = wb_o.at[j, dp]
        return (
            pltpu.make_async_copy(wst.at[s], dst, w_loc.at[s]),
            remote(wst.at[s], dst, w_par.at[s], wp_recv.at[j], partner),
            remote(wst.at[s], dst, w_nbr.at[s], wx_recv.at[j], nbr),
        )

    def tail_copies(w):
        s = rem(w, DEVS)
        for ref, (first, count, row, rows) in zip((tail_0, tail_1, tail_2, tail_3, tail_4), TAILS):
            low = HEAD + first
            yield low, low + count, lambda ref=ref, low=low, row=row, rows=rows: pltpu.make_async_copy(
                wst.at[s, pl.ds(row, rows), :], ref.at[w - low], w_loc.at[s]
            )

    def mid_copy():
        return remote(wst.at[0], mid.at[0], w_nbr.at[0], mid_recv.at[0], nbr)

    def f_mat(w):
        return lax.div(w, DEVS) * DEVS + owner_of(*shifted(y, nbr_dp, rem(w, DEVS)))

    def f_copy(w):
        j = f_mat(w)
        ref = wb_o.at[j, nbr_dp]
        return remote(ref, ref, f_send.at[j], f_recv.at[j], partner)

    def presum(t):
        own_copy(t).wait()
        a_copy(t).wait_recv()

        @pl.when(t >= LAG)
        def _():
            rs_copy(t - LAG).wait_send()

        so, sa, ss = rem(t, 2), rem(t, A_SLOTS), rem(t, LAG)

        def body(rows):
            sendb[ss, rows, :] = own[so, 1 - x, rows, :] + ra[sa, 1 - x, rows, :]
            acc[ss, rows, :] = own[so, x, rows, :] + ra[sa, x, rows, :]

        row_loop(RB, body)
        rs_copy(t).start()

        @pl.when(t + 2 < MATS)
        def _():
            own_copy(t + 2).start()

        @pl.when(t + LEAD < MATS)
        def _():
            @pl.when(t + LEAD > A_SLOTS)
            def _():
                a_copy(t + LEAD - A_SLOTS).wait_send()

            a_copy(t + LEAD).start()

    def piece_copy(q):
        if q == PIECES:
            src, dst = grad.at[0, x, 1 - c], ra.at[0, x]
        else:
            rows = pl.ds(q * PIECE, PIECE)
            src, dst = wtq.at[0, rows, :], ra.at[0, 1 - x, rows, :]
        return remote(src, dst, p_send.at[q], p_recv.at[q], partner)

    def stage_copy():
        return pltpu.make_async_copy(grad.at[0, 1 - x, 1 - c], wtq.at[0], wtq_sem.at[0])

    def presum_first():
        own_copy(0).wait()
        for q in range(PIECES):
            piece_copy(q).wait_recv()
            rows = pl.ds(q * PIECE, PIECE)
            sendb[0, rows, :] = own[0, 1 - x, rows, :] + ra[0, 1 - x, rows, :]
            remote(
                sendb.at[0, rows, :], recvb.at[0, rows, :], rs_send.at[0], rs_recv.at[0], nbr
            ).start()
        piece_copy(PIECES).wait_recv()

        def body(rows):
            acc[0, rows, :] = own[0, x, rows, :] + ra[0, x, rows, :]

        row_loop(RB, body)
        own_copy(2).start()
        a_copy(LEAD).start()
        for q in range(PIECES + 1):
            piece_copy(q).wait_send()

    def finish(j):
        mom_load(j).wait()

        @pl.when(j >= 2)
        def _():
            mom_store(j - 2).wait()

        k = rem(j, DEVS)
        r = lax.div(j, DEVS)

        @pl.when((j >= DEVS) & (k != me))
        def _():
            u_copy(j - DEVS).wait_send()

        rs_copy(j).wait_recv()
        sm, ss, sr = rem(j, 2), rem(j, LAG), rem(j, B_SLOTS)

        def body(rows):
            mean = (acc[ss, rows, :] + recvb[sr, rows, :]) * 0.25
            new = MOMENTUM * momi[sm, rows, :] + mean
            momq[sm, rows, :] = new
            ust[k, rows, :] = (mean + MOMENTUM * new).astype(BF16)

        row_loop(RB, body)

        @pl.when(k != me)
        def _():
            u_copy(j).start()

        mom_store(j).start()

        @pl.when(j + 2 < MATS)
        def _():
            mom_load(j + 2).start()

        for half in range(2):
            @pl.when((k == me) & (y == half))
            def _():
                def put(rows):
                    dst = pl.ds(pl.multiple_of(dp * RB + rows.start, CHUNK), CHUNK)
                    xb[r, dst, half * CB:(half + 1) * CB] = ust[k, rows, :]

                row_loop(RB, put)

    def normalize(r):
        def square(i, total):
            v = xb[r, pl.ds(pl.multiple_of(i * CHUNK, CHUNK), CHUNK), :].astype(F32)
            return total + jnp.sum((v * v).reshape(CHUNK // 8, 8, COLS), axis=0)

        total = lax.fori_loop(0, ROWS // CHUNK, square, jnp.zeros((8, COLS), F32))
        norm = jnp.sqrt(jnp.sum(total, keepdims=True)) + NORM_EPS

        def scale(rows):
            xb[r, rows, :] = (xb[r, rows, :].astype(F32) / norm).astype(BF16)

        row_loop(ROWS, scale)

    def iterate(r):
        @pl.loop(0, COLS // 256)
        def _(m):
            cols = pl.ds(pl.multiple_of(m * 256, 256), 256)
            gram[cols, :] = lax.dot_general(
                xb[r, :, cols], xb[r], (((0,), (0,)), ((), ())), preferred_element_type=F32
            ).astype(BF16)

        @pl.loop(0, COLS // 256)
        def _(m):
            rows = pl.ds(pl.multiple_of(m * 256, 256), 256)
            part = gram[rows, :]
            square = jnp.dot(part, gram[...], preferred_element_type=F32)
            poly[rows, :] = (COEF_B * part.astype(F32) + COEF_C * square).astype(BF16)

        @pl.loop(0, ROWS // 512)
        def _(m):
            rows = pl.ds(pl.multiple_of(m * 512, 512), 512)
            part = xb[r, rows, :]
            prod = jnp.dot(part, poly[...], preferred_element_type=F32)
            xb[r, rows, :] = (COEF_A * part.astype(F32) + prod).astype(BF16)

    def ortho(r, s):
        @pl.when(s == 0)
        def _():
            @pl.loop(1, DEVS)
            def _(i):
                yy, dd = coords(i)
                remote(
                    ust.at[0], xblock(r, dd, yy), u_send.at[0],
                    u_recv.at[r * DEVS + owner_of(yy, dd)], partner,
                ).wait_recv()

            normalize(r)

        iterate(r)

        @pl.when(s == NS_STEPS - 1)
        def _():
            @pl.loop(0, DEVS)
            def _(n):
                i = rem(n + 4, DEVS)

                @pl.when(i != 0)
                def _():
                    x_copy(r, i).start()

            for half in range(2):
                @pl.when(y == half)
                def _():
                    def put(rows):
                        src = pl.ds(pl.multiple_of(dp * RB + rows.start, CHUNK), CHUNK)
                        rx[r * DEVS + me, rows, :] = xb[r, src, half * CB:(half + 1) * CB]

                    row_loop(RB, put)

    def forward(w):
        f_copy_in = remote(
            wst.at[0], wb_o.at[f_mat(w), nbr_dp], w_nbr.at[0], wx_recv.at[f_mat(w)], nbr
        )
        f_copy_in.wait_recv()
        f_copy(w).start()

    def weights(w):
        j = w_mat(w)

        @pl.when(rem(w, DEVS) != 0)
        def _():
            remote(xblock(0, 0, 0), rx.at[j], x_send.at[0], x_recv.at[j], nbr).wait_recv()

        wt_load(w).wait()

        @pl.when(w >= 2)
        def _():
            wt_store(w - 2).wait()

        @pl.when(w >= DEVS)
        def _():
            old = w_copies(w - DEVS)
            old[0].wait()
            old[1].wait_send()
            old[2].wait_send()

        s2, s8 = rem(w, 2), rem(w, DEVS)
        lr = rate[j]
        wd = decay[...]

        def body(rows):
            cur = wti[s2, rows, :]
            new = cur - lr * (OUT_SCALE * rx[j, rows, :].astype(F32) + wd * cur)
            wtq[s2, rows, :] = new
            wst[s8, rows, :] = new.astype(BF16)

        row_loop(RB, body)

        @pl.when(w < HEAD)
        def _():
            now = w_copies(w)
            now[2].start()
            now[1].start()
            now[0].start()

        for low, high, copy in tail_copies(w):
            @pl.when((w >= low) & (w < high))
            def _():
                copy().start()

        @pl.when(w == HEAD)
        def _():
            mid_copy().start()

        wt_store(w).start()

        @pl.when(w + 2 < MATS)
        def _():
            wt_load(w + 2).start()

        @pl.when((w >= DEVS) & (w < HEAD))
        def _():
            forward(w - DEVS)

    barrier = pltpu.get_barrier_semaphore()
    for i in range(1, DEVS):
        yy, dd = coords(i)
        pl.semaphore_signal(barrier, inc=1, device_id={"tp": yy, "dp": dd}, device_id_type=MESH)
    stage_copy().start()
    own_copy(0).start()
    pl.semaphore_wait(barrier, DEVS - 1)

    stage_copy().wait()
    for q in range(PIECES + 1):
        piece_copy(q).start()
    for t in range(1, LEAD):
        a_copy(t).start()
    own_copy(1).start()
    rate_copy().start()
    for t in range(2):
        mom_load(t).start()
        wt_load(t).start()
    presum_first()
    rate_copy().wait()

    def w_done(t):
        return (
            jnp.minimum(4 * jnp.clip(t - W_START[0], 0, 1) + 2 * jnp.clip(t - W_START[0] - 1, 0, 2), 8)
            + jnp.minimum(4 * jnp.clip(t - W_START[1], 0, 1) + 2 * jnp.clip(t - W_START[1] - 1, 0, 2), 8)
        )

    @pl.loop(0, STEPS)
    def _(t):
        @pl.when((t >= LAG) & (t < MATS + LAG))
        def _():
            finish(t - LAG)

        @pl.when((t >= 1) & (t < MATS))
        def _():
            presum(t)

        pl.loop(w_done(t), w_done(t + 1))(weights)

        r = jnp.where(t >= NS_START[2], 2, jnp.where(t >= NS_START[1], 1, 0))
        base = jnp.where(
            t >= NS_START[2], NS_START[2], jnp.where(t >= NS_START[1], NS_START[1], NS_START[0])
        )

        @pl.when((t >= base) & (t < base + NS_STEPS))
        def _():
            ortho(r, t - base)

    @pl.loop(HEAD - DEVS, HEAD)
    def _(w):
        forward(w)

    for t in range(MATS - LAG, MATS):
        rs_copy(t).wait_send()
    for t in range(MATS - A_SLOTS, MATS):
        a_copy(t).wait_send()
    for j in range(MATS - 2, MATS):
        mom_store(j).wait()

    @pl.loop(HEAD, MATS)
    def _(j):
        @pl.when(rem(j, DEVS) != me)
        def _():
            u_copy(j).wait_send()

    def drain_x(r):
        @pl.loop(1, DEVS)
        def _(i):
            x_copy(r, i).wait_send()

    pl.loop(0, ROUNDS - 1)(drain_x)

    @pl.loop(0, HEAD)
    def _(w):
        j = w_mat(w)
        remote(wst.at[0], wb_o.at[j, dp], w_par.at[0], wp_recv.at[j], partner).wait_recv()
        f_copy(w).wait_send()
        ref = wb_o.at[j, 3 - dp]
        remote(ref, ref, f_send.at[j], f_recv.at[j], partner).wait_recv()

    pl.loop(HEAD, MATS)(weights)
    drain_x(ROUNDS - 1)
    for w in range(HEAD, MATS):
        pltpu.make_async_copy(wst.at[0], tail_0.at[0], w_loc.at[w % DEVS]).wait()
    for w in range(MATS - 2, MATS):
        wt_store(w).wait()
    mid_copy().wait()


def publish_kernel(mom, wt, wb, mom_o, wt_o, wb_o):
    mom_o[...] = mom[...]
    wt_o[...] = wt[...]
    wb_o[...] = wb[...]


def publish(mom, wt, wb):
    steps = HEAD
    small = pl.BlockSpec((MATS * RB // steps, CB), lambda i: (i, 0))
    large = pl.BlockSpec((ROWS, CB), lambda i: (i, 0))
    return pl.pallas_call(
        publish_kernel,
        name="publish",
        grid=(steps,),
        out_shape=(
            jax.ShapeDtypeStruct((MATS * RB, CB), F32),
            jax.ShapeDtypeStruct((MATS * RB, CB), F32),
            jax.ShapeDtypeStruct((MATS * ROWS, CB), BF16),
        ),
        in_specs=[small, small, large],
        out_specs=[small, small, large],
        cost_estimate=pl.CostEstimate(
            flops=40_000_000_000, bytes_accessed=126_000_000, transcendentals=0
        ),
        compiler_params=pltpu.CompilerParams(vmem_limit_bytes=44 << 20),
    )(mom.reshape(-1, CB), wt.reshape(-1, CB), wb.reshape(-1, CB))


def fill_kernel(tail, own, par, nbr, fwd, whole, out, sems):
    dp = lax.axis_index("dp")
    y = lax.axis_index("tp")
    places = (dp, dp + 1 - 2 * rem(dp, 2), rem(dp + 2, 4), 3 - dp)
    copies = [
        pltpu.make_async_copy(
            ref.at[i],
            out.at[HEAD + owner_of(*shifted(y, place, tail[0] + i)), place, pl.ds(tail[2], tail[3]), :],
            sems.at[n, i],
        )
        for n, (ref, place) in enumerate(zip((own, par, nbr, fwd), places))
        for i in range(own.shape[0])
    ]
    for copy in copies:
        copy.start()
    for copy in copies:
        copy.wait()


def fill(whole, tail, own, par, nbr, fwd):
    count = own.shape[0]
    hbm = pl.BlockSpec(memory_space=pl.ANY)
    return pl.pallas_call(
        functools.partial(fill_kernel, tail),
        name="fill",
        out_shape=jax.ShapeDtypeStruct(whole.shape, whole.dtype),
        in_specs=[pl.BlockSpec(memory_space=pltpu.VMEM)] * 4 + [hbm],
        out_specs=hbm,
        scratch_shapes=[pltpu.SemaphoreType.DMA((4, count))],
        input_output_aliases={4: 0},
        compiler_params=pltpu.CompilerParams(vmem_limit_bytes=10 << 20),
        cost_estimate=pl.CostEstimate(
            flops=count * 1_000_000_000, bytes_accessed=count * 3_200_000, transcendentals=0
        ),
    )(own, par, nbr, fwd, whole)


def solution(mesh):
    def local_step(grad_local, mom_local, weight_local, learn_rate, decay_rate):
        hbm = pl.BlockSpec(memory_space=pl.ANY)
        dma = pltpu.SemaphoreType.DMA
        block = (RB, CB)
        mom_new, weight_new, head, *tails, mid = pl.pallas_call(
            kernel,
            name="muon_step",
            out_shape=(
                jax.ShapeDtypeStruct((MATS,) + block, F32),
                jax.ShapeDtypeStruct((MATS,) + block, F32),
                jax.ShapeDtypeStruct((HEAD, 4) + block, BF16),
            )
            + tuple(jax.ShapeDtypeStruct((n, rows, CB), BF16) for _, n, _, rows in TAILS)
            + (jax.ShapeDtypeStruct((1,) + block, BF16),),
            in_specs=[hbm] * 4 + [pl.BlockSpec(memory_space=pltpu.SMEM)],
            out_specs=[hbm] * (4 + len(TAILS)),
            scratch_shapes=[
                pltpu.SMEM((MATS,), F32),
                dma((1,)),
                pltpu.VMEM((2, 2) + block, F32),
                pltpu.VMEM((A_SLOTS, 2) + block, F32),
                pltpu.VMEM((LAG,) + block, F32),
                pltpu.VMEM((B_SLOTS,) + block, F32),
                pltpu.VMEM((LAG,) + block, F32),
                pltpu.VMEM((2,) + block, F32),
                pltpu.VMEM((2,) + block, F32),
                pltpu.VMEM((2,) + block, F32),
                pltpu.VMEM((2,) + block, F32),
                pltpu.VMEM((DEVS,) + block, BF16),
                pltpu.VMEM((DEVS,) + block, BF16),
                pltpu.VMEM((ROUNDS, ROWS, COLS), BF16),
                pltpu.VMEM((MATS,) + block, BF16),
                pltpu.VMEM((COLS, COLS), BF16),
                pltpu.VMEM((COLS, COLS), BF16),
                dma((1,)), dma((PIECES + 1,)), dma((PIECES + 1,)),
                dma((2,)), dma((A_SLOTS,)), dma((A_SLOTS,)), dma((LAG,)), dma((B_SLOTS,)),
                dma((2,)), dma((2,)), dma((2,)), dma((2,)),
                dma((DEVS,)), dma((MATS,)), dma((MATS,)), dma((MATS,)),
                dma((DEVS,)), dma((DEVS,)), dma((DEVS,)), dma((MATS,)), dma((MATS,)),
                dma((MATS,)), dma((MATS,)),
            ],
            compiler_params=pltpu.CompilerParams(
                collective_id=0, has_side_effects=True, vmem_limit_bytes=67_000_000
            ),
            cost_estimate=pl.CostEstimate(
                flops=3 * 28_700_000_000, bytes_accessed=400_000_000, transcendentals=0
            ),
        )(
            grad_local.reshape((MATS, 2, 2) + block),
            mom_local,
            weight_local,
            learn_rate,
            decay_rate,
        )
        across = [(0, 2), (1, 3), (2, 0), (3, 1)]
        beside = [(0, 1), (1, 0), (2, 3), (3, 2)]

        def move(value, pairs):
            return lax.ppermute(value, "dp", pairs)

        nbr = [mid] + [move(tails[n], across) for n in range(1, len(tails))]
        par = [move(part, beside) for part in tails]
        fwd = [move(part, beside) for part in nbr]
        mom_new, weight_new, full = publish(mom_new, weight_new, head)
        full = full.reshape((MATS, 4) + block)
        for n, part in enumerate(tails):
            full = fill(full, TAILS[n], part, par[n], nbr[n], fwd[n])
        return (
            mom_new.reshape((MATS,) + block),
            weight_new.reshape((MATS,) + block),
            full.reshape(MATS, ROWS, CB),
        )

    return jax.shard_map(
        local_step,
        mesh=mesh,
        in_specs=(P(("rep", "dp"), None, None, "tp"), P("rep", "dp", "tp"), P("rep", "dp", "tp"), P("rep"), P()),
        out_specs=(P("rep", "dp", "tp"), P("rep", "dp", "tp"), P("rep", None, "tp")),
        check_vma=False,
    )
```

```python
import functools
import math

import jax
import jax.numpy as jnp
from jax import lax
from jax.experimental import pallas as pl
from jax.experimental.pallas import tpu as pltpu
from jax.sharding import PartitionSpec as P


MOMENTUM = 0.95
NS_STEPS = 5
COEF_A = 3.4445
COEF_B = -4.7750
COEF_C = 2.0315
NORM_EPS = 1e-7

MESH = pl.DeviceIdType.MESH
F32 = jnp.float32
BF16 = jnp.bfloat16

MATS = 24
ROWS = 2048
COLS = 768
DEVS = 8
ROUNDS = MATS // DEVS
RB = ROWS // 4
CB = COLS // 2
OUT_SCALE = 0.2 * math.sqrt(max(ROWS, COLS))

LAG = 3
LEAD = 2
A_SLOTS = 2 * LEAD
B_SLOTS = 2 * LAG
NS_START = (8 + LAG + 2, 16 + LAG + 2, 24 + LAG)
W_START = (NS_START[0] + 7, NS_START[2])
STEPS = NS_START[2] + NS_STEPS
CHUNK = 64
HEAD = MATS - DEVS
TAILS = ((0, 1, 0, RB), (1, 4, 0, RB), (5, 2, 0, RB), (7, 1, 0, RB // 2), (7, 1, RB // 2, RB // 2))
PIECES = ((0, 64), (64, 64), (128, 128), (256, 256))
LAST = len(PIECES)


def rem(a, b):
    return lax.rem(a, b)


def owner_of(yy, dd):
    return yy * 4 + rem(dd, 2) * 2 + lax.div(dd, 2)


def shifted(yy, dd, i):
    dx, dy, dc = lax.div(i, 4), rem(lax.div(i, 2), 2), rem(i, 2)
    xx = rem(lax.div(dd, 2) + dx, 2)
    return rem(yy + dy, 2), xx * 2 + rem(rem(dd, 2) + dc, 2)


def row_loop(total, body):
    @pl.loop(0, total // CHUNK)
    def _(i):
        body(pl.ds(pl.multiple_of(i * CHUNK, CHUNK), CHUNK))


def kernel(
    grad, mom, wt, rate_in, decay,
    mom_o, wt_o, wb_o, tail_0, tail_1, tail_2, tail_3, tail_4, mid,
    rate, rate_sem, own, ra, sendb, recvb, acc, momi, momq, wti, wtq, ust, wst, xb, rx, gram, poly,
    mid_recv, p_send, p_recv, own_sem, a_send, a_recv, rs_send, rs_recv, momi_sem, momq_sem, wti_sem, wtq_sem,
    u_send, u_recv, x_send, x_recv, w_loc, w_par, w_nbr, wp_recv, wx_recv, f_send, f_recv,
):
    dp = lax.axis_index("dp")
    y = lax.axis_index("tp")
    x = lax.div(dp, 2)
    c = rem(dp, 2)
    me = owner_of(y, dp)
    partner = {"tp": y, "dp": x * 2 + (1 - c)}
    nbr_dp = (1 - x) * 2 + c
    nbr = {"tp": y, "dp": nbr_dp}

    def coords(i):
        return shifted(y, dp, i)

    def remote(src, dst, ss, rs, dev):
        return pltpu.make_async_remote_copy(
            src_ref=src, dst_ref=dst, send_sem=ss, recv_sem=rs, device_id=dev, device_id_type=MESH
        )

    def xblock(r, dd, yy):
        return xb.at[
            r, pl.ds(pl.multiple_of(dd * RB, RB), RB), pl.ds(pl.multiple_of(yy * CB, CB), CB)
        ]

    def rate_copy():
        return pltpu.make_async_copy(rate_in, rate, rate_sem.at[0])

    def own_copy(t):
        s = rem(t, 2)
        return pltpu.make_async_copy(grad.at[t, :, c], own.at[s], own_sem.at[s])

    def a_copy(t):
        s = rem(t, A_SLOTS)
        return remote(grad.at[t, :, 1 - c], ra.at[s], a_send.at[s], a_recv.at[s], partner)

    def rs_copy(t):
        s, d = rem(t, LAG), rem(t, B_SLOTS)
        return remote(sendb.at[s], recvb.at[d], rs_send.at[s], rs_recv.at[d], nbr)

    def mom_load(j):
        s = rem(j, 2)
        return pltpu.make_async_copy(mom.at[j], momi.at[s], momi_sem.at[s])

    def mom_store(j):
        s = rem(j, 2)
        return pltpu.make_async_copy(momq.at[s], mom_o.at[j], momq_sem.at[s])

    def u_copy(j):
        k = rem(j, DEVS)
        r = lax.div(j, DEVS)
        dev = {"tp": lax.div(k, 4), "dp": rem(k, 2) * 2 + rem(lax.div(k, 2), 2)}
        return remote(ust.at[k], xblock(r, dp, y), u_send.at[k], u_recv.at[r * DEVS + me], dev)

    def x_copy(r, i):
        yy, dd = coords(i)
        j = r * DEVS + me
        return remote(
            xblock(r, dd, yy), rx.at[j], x_send.at[r * DEVS + i], x_recv.at[j], {"tp": yy, "dp": dd}
        )

    def w_mat(w):
        return lax.div(w, DEVS) * DEVS + owner_of(*coords(rem(w, DEVS)))

    def wt_load(w):
        s = rem(w, 2)
        return pltpu.make_async_copy(wt.at[w_mat(w)], wti.at[s], wti_sem.at[s])

    def wt_store(w):
        s = rem(w, 2)
        return pltpu.make_async_copy(wtq.at[s], wt_o.at[w_mat(w)], wtq_sem.at[s])

    def w_copies(w):
        j, s = w_mat(w), rem(w, DEVS)
        dst = wb_o.at[j, dp]
        return (
            pltpu.make_async_copy(wst.at[s], dst, w_loc.at[s]),
            remote(wst.at[s], dst, w_par.at[s], wp_recv.at[j], partner),
            remote(wst.at[s], dst, w_nbr.at[s], wx_recv.at[j], nbr),
        )

    def tail_copies(w):
        s = rem(w, DEVS)
        for ref, (first, count, row, rows) in zip((tail_0, tail_1, tail_2, tail_3, tail_4), TAILS):
            low = HEAD + first
            yield low, low + count, lambda ref=ref, low=low, row=row, rows=rows: pltpu.make_async_copy(
                wst.at[s, pl.ds(row, rows), :], ref.at[w - low], w_loc.at[s]
            )

    def mid_copy():
        return remote(wst.at[0], mid.at[0], w_nbr.at[0], mid_recv.at[0], nbr)

    def f_mat(w):
        return lax.div(w, DEVS) * DEVS + owner_of(*shifted(y, nbr_dp, rem(w, DEVS)))

    def f_copy(w):
        j = f_mat(w)
        ref = wb_o.at[j, nbr_dp]
        return remote(ref, ref, f_send.at[j], f_recv.at[j], partner)

    def presum(t):
        own_copy(t).wait()
        a_copy(t).wait_recv()

        @pl.when(t >= LAG)
        def _():
            rs_copy(t - LAG).wait_send()

        so, sa, ss = rem(t, 2), rem(t, A_SLOTS), rem(t, LAG)

        def body(rows):
            sendb[ss, rows, :] = own[so, 1 - x, rows, :] + ra[sa, 1 - x, rows, :]
            acc[ss, rows, :] = own[so, x, rows, :] + ra[sa, x, rows, :]

        row_loop(RB, body)
        rs_copy(t).start()

        @pl.when(t + 2 < MATS)
        def _():
            own_copy(t + 2).start()

        @pl.when(t + LEAD < MATS)
        def _():
            @pl.when(t + LEAD > A_SLOTS)
            def _():
                a_copy(t + LEAD - A_SLOTS).wait_send()

            a_copy(t + LEAD).start()

    def piece_copy(q):
        if q == LAST:
            src, dst = grad.at[0, x, 1 - c], ra.at[0, x]
        else:
            rows = pl.ds(*PIECES[q])
            src, dst = wtq.at[0, rows, :], ra.at[0, 1 - x, rows, :]
        return remote(src, dst, p_send.at[q], p_recv.at[q], partner)

    def stage_copy():
        return pltpu.make_async_copy(grad.at[0, 1 - x, 1 - c], wtq.at[0], wtq_sem.at[0])

    def presum_first():
        own_copy(0).wait()
        for q in range(LAST):
            piece_copy(q).wait_recv()
            rows = pl.ds(*PIECES[q])
            sendb[0, rows, :] = own[0, 1 - x, rows, :] + ra[0, 1 - x, rows, :]
            remote(
                sendb.at[0, rows, :], recvb.at[0, rows, :], rs_send.at[0], rs_recv.at[0], nbr
            ).start()
            if q == 0:
                piece_copy(LAST).start()
                for t in range(1, LEAD):
                    a_copy(t).start()
                own_copy(1).start()
                rate_copy().start()
                for t in range(2):
                    mom_load(t).start()
                    wt_load(t).start()
        piece_copy(LAST).wait_recv()

        def body(rows):
            acc[0, rows, :] = own[0, x, rows, :] + ra[0, x, rows, :]

        row_loop(RB, body)
        own_copy(2).start()
        a_copy(LEAD).start()
        for q in range(LAST + 1):
            piece_copy(q).wait_send()

    def finish(j):
        mom_load(j).wait()

        @pl.when(j >= 2)
        def _():
            mom_store(j - 2).wait()

        k = rem(j, DEVS)
        r = lax.div(j, DEVS)

        @pl.when((j >= DEVS) & (k != me))
        def _():
            u_copy(j - DEVS).wait_send()

        rs_copy(j).wait_recv()
        sm, ss, sr = rem(j, 2), rem(j, LAG), rem(j, B_SLOTS)

        def body(rows):
            mean = (acc[ss, rows, :] + recvb[sr, rows, :]) * 0.25
            new = MOMENTUM * momi[sm, rows, :] + mean
            momq[sm, rows, :] = new
            ust[k, rows, :] = (mean + MOMENTUM * new).astype(BF16)

        row_loop(RB, body)

        @pl.when(k != me)
        def _():
            u_copy(j).start()

        mom_store(j).start()

        @pl.when(j + 2 < MATS)
        def _():
            mom_load(j + 2).start()

        for half in range(2):
            @pl.when((k == me) & (y == half))
            def _():
                def put(rows):
                    dst = pl.ds(pl.multiple_of(dp * RB + rows.start, CHUNK), CHUNK)
                    xb[r, dst, half * CB:(half + 1) * CB] = ust[k, rows, :]

                row_loop(RB, put)

    def normalize(r):
        def square(i, total):
            v = xb[r, pl.ds(pl.multiple_of(i * CHUNK, CHUNK), CHUNK), :].astype(F32)
            return total + jnp.sum((v * v).reshape(CHUNK // 8, 8, COLS), axis=0)

        total = lax.fori_loop(0, ROWS // CHUNK, square, jnp.zeros((8, COLS), F32))
        norm = jnp.sqrt(jnp.sum(total, keepdims=True)) + NORM_EPS

        def scale(rows):
            xb[r, rows, :] = (xb[r, rows, :].astype(F32) / norm).astype(BF16)

        row_loop(ROWS, scale)

    def iterate(r):
        @pl.loop(0, COLS // 256)
        def _(m):
            cols = pl.ds(pl.multiple_of(m * 256, 256), 256)
            gram[cols, :] = lax.dot_general(
                xb[r, :, cols], xb[r], (((0,), (0,)), ((), ())), preferred_element_type=F32
            ).astype(BF16)

        @pl.loop(0, COLS // 256)
        def _(m):
            rows = pl.ds(pl.multiple_of(m * 256, 256), 256)
            part = gram[rows, :]
            square = jnp.dot(part, gram[...], preferred_element_type=F32)
            poly[rows, :] = (COEF_B * part.astype(F32) + COEF_C * square).astype(BF16)

        @pl.loop(0, ROWS // 512)
        def _(m):
            rows = pl.ds(pl.multiple_of(m * 512, 512), 512)
            part = xb[r, rows, :]
            prod = jnp.dot(part, poly[...], preferred_element_type=F32)
            xb[r, rows, :] = (COEF_A * part.astype(F32) + prod).astype(BF16)

    def ortho(r, s):
        @pl.when(s == 0)
        def _():
            @pl.loop(1, DEVS)
            def _(i):
                yy, dd = coords(i)
                remote(
                    ust.at[0], xblock(r, dd, yy), u_send.at[0],
                    u_recv.at[r * DEVS + owner_of(yy, dd)], partner,
                ).wait_recv()

            normalize(r)

        iterate(r)

        @pl.when(s == NS_STEPS - 1)
        def _():
            @pl.loop(0, DEVS)
            def _(n):
                i = rem(n + 4, DEVS)

                @pl.when(i != 0)
                def _():
                    x_copy(r, i).start()

            for half in range(2):
                @pl.when(y == half)
                def _():
                    def put(rows):
                        src = pl.ds(pl.multiple_of(dp * RB + rows.start, CHUNK), CHUNK)
                        rx[r * DEVS + me, rows, :] = xb[r, src, half * CB:(half + 1) * CB]

                    row_loop(RB, put)

    def forward(w):
        f_copy_in = remote(
            wst.at[0], wb_o.at[f_mat(w), nbr_dp], w_nbr.at[0], wx_recv.at[f_mat(w)], nbr
        )
        f_copy_in.wait_recv()
        f_copy(w).start()

    def weights(w):
        j = w_mat(w)

        @pl.when(rem(w, DEVS) != 0)
        def _():
            remote(xblock(0, 0, 0), rx.at[j], x_send.at[0], x_recv.at[j], nbr).wait_recv()

        wt_load(w).wait()

        @pl.when(w >= 2)
        def _():
            wt_store(w - 2).wait()

        @pl.when(w >= DEVS)
        def _():
            old = w_copies(w - DEVS)
            old[0].wait()
            old[1].wait_send()
            old[2].wait_send()

        s2, s8 = rem(w, 2), rem(w, DEVS)
        lr = rate[j]
        wd = decay[...]

        def body(rows):
            cur = wti[s2, rows, :]
            new = cur - lr * (OUT_SCALE * rx[j, rows, :].astype(F32) + wd * cur)
            wtq[s2, rows, :] = new
            wst[s8, rows, :] = new.astype(BF16)

        row_loop(RB, body)

        @pl.when(w < HEAD)
        def _():
            now = w_copies(w)
            now[2].start()
            now[1].start()
            now[0].start()

        for low, high, copy in tail_copies(w):
            @pl.when((w >= low) & (w < high))
            def _():
                copy().start()

        @pl.when(w == HEAD)
        def _():
            mid_copy().start()

        wt_store(w).start()

        @pl.when(w + 2 < MATS)
        def _():
            wt_load(w + 2).start()

        @pl.when((w >= DEVS) & (w < HEAD))
        def _():
            forward(w - DEVS)

    barrier = pltpu.get_barrier_semaphore()
    beside = dp + 1 - 2 * c
    peers = [(1 - y, dd) for dd in (3 - dp, nbr_dp, dp, beside)]
    for yy, dd in peers + [(y, dd) for dd in (3 - dp, nbr_dp, beside)]:
        pl.semaphore_signal(barrier, inc=1, device_id={"tp": yy, "dp": dd}, device_id_type=MESH)
    stage_copy().start()
    own_copy(0).start()
    pl.semaphore_wait(barrier, DEVS - 1)

    stage_copy().wait()
    for q in range(LAST):
        piece_copy(q).start()
    presum_first()
    rate_copy().wait()

    def w_done(t):
        return (
            jnp.minimum(4 * jnp.clip(t - W_START[0], 0, 1) + 2 * jnp.clip(t - W_START[0] - 1, 0, 2), 8)
            + jnp.minimum(4 * jnp.clip(t - W_START[1], 0, 1) + 2 * jnp.clip(t - W_START[1] - 1, 0, 2), 8)
        )

    @pl.loop(0, STEPS)
    def _(t):
        @pl.when((t >= LAG) & (t < MATS + LAG))
        def _():
            finish(t - LAG)

        @pl.when((t >= 1) & (t < MATS))
        def _():
            presum(t)

        pl.loop(w_done(t), w_done(t + 1))(weights)

        r = jnp.where(t >= NS_START[2], 2, jnp.where(t >= NS_START[1], 1, 0))
        base = jnp.where(
            t >= NS_START[2], NS_START[2], jnp.where(t >= NS_START[1], NS_START[1], NS_START[0])
        )

        @pl.when((t >= base) & (t < base + NS_STEPS))
        def _():
            ortho(r, t - base)

    @pl.loop(HEAD - DEVS, HEAD)
    def _(w):
        forward(w)

    for t in range(MATS - LAG, MATS):
        rs_copy(t).wait_send()
    for t in range(MATS - A_SLOTS, MATS):
        a_copy(t).wait_send()
    for j in range(MATS - 2, MATS):
        mom_store(j).wait()

    @pl.loop(HEAD, MATS)
    def _(j):
        @pl.when(rem(j, DEVS) != me)
        def _():
            u_copy(j).wait_send()

    def drain_x(r):
        @pl.loop(1, DEVS)
        def _(i):
            x_copy(r, i).wait_send()

    pl.loop(0, ROUNDS - 1)(drain_x)

    @pl.loop(0, HEAD)
    def _(w):
        j = w_mat(w)
        remote(wst.at[0], wb_o.at[j, dp], w_par.at[0], wp_recv.at[j], partner).wait_recv()
        f_copy(w).wait_send()
        ref = wb_o.at[j, 3 - dp]
        remote(ref, ref, f_send.at[j], f_recv.at[j], partner).wait_recv()

    pl.loop(HEAD, MATS)(weights)
    drain_x(ROUNDS - 1)
    for w in range(HEAD, MATS):
        pltpu.make_async_copy(wst.at[0], tail_0.at[0], w_loc.at[w % DEVS]).wait()
    for w in range(MATS - 2, MATS):
        wt_store(w).wait()
    mid_copy().wait()


def publish_kernel(mom, wt, wb, mom_o, wt_o, wb_o):
    mom_o[...] = mom[...]
    wt_o[...] = wt[...]
    wb_o[...] = wb[...]


def publish(mom, wt, wb):
    steps = HEAD
    small = pl.BlockSpec((MATS * RB // steps, CB), lambda i: (i, 0))
    large = pl.BlockSpec((ROWS, CB), lambda i: (i, 0))
    return pl.pallas_call(
        publish_kernel,
        name="publish",
        grid=(steps,),
        out_shape=(
            jax.ShapeDtypeStruct((MATS * RB, CB), F32),
            jax.ShapeDtypeStruct((MATS * RB, CB), F32),
            jax.ShapeDtypeStruct((MATS * ROWS, CB), BF16),
        ),
        in_specs=[small, small, large],
        out_specs=[small, small, large],
        cost_estimate=pl.CostEstimate(
            flops=40_000_000_000, bytes_accessed=126_000_000, transcendentals=0
        ),
        compiler_params=pltpu.CompilerParams(vmem_limit_bytes=44 << 20),
    )(mom.reshape(-1, CB), wt.reshape(-1, CB), wb.reshape(-1, CB))


def fill_kernel(tail, own, par, nbr, fwd, whole, out, sems):
    dp = lax.axis_index("dp")
    y = lax.axis_index("tp")
    places = (dp, dp + 1 - 2 * rem(dp, 2), rem(dp + 2, 4), 3 - dp)
    copies = [
        pltpu.make_async_copy(
            ref.at[i],
            out.at[HEAD + owner_of(*shifted(y, place, tail[0] + i)), place, pl.ds(tail[2], tail[3]), :],
            sems.at[n, i],
        )
        for n, (ref, place) in enumerate(zip((own, par, nbr, fwd), places))
        for i in range(own.shape[0])
    ]
    for copy in copies:
        copy.start()
    for copy in copies:
        copy.wait()


def fill(whole, tail, own, par, nbr, fwd):
    count = own.shape[0]
    hbm = pl.BlockSpec(memory_space=pl.ANY)
    return pl.pallas_call(
        functools.partial(fill_kernel, tail),
        name="fill",
        out_shape=jax.ShapeDtypeStruct(whole.shape, whole.dtype),
        in_specs=[pl.BlockSpec(memory_space=pltpu.VMEM)] * 4 + [hbm],
        out_specs=hbm,
        scratch_shapes=[pltpu.SemaphoreType.DMA((4, count))],
        input_output_aliases={4: 0},
        compiler_params=pltpu.CompilerParams(vmem_limit_bytes=10 << 20),
        cost_estimate=pl.CostEstimate(
            flops=count * 1_000_000_000, bytes_accessed=count * 3_200_000, transcendentals=0
        ),
    )(own, par, nbr, fwd, whole)


def solution(mesh):
    def local_step(grad_local, mom_local, weight_local, learn_rate, decay_rate):
        hbm = pl.BlockSpec(memory_space=pl.ANY)
        dma = pltpu.SemaphoreType.DMA
        block = (RB, CB)
        mom_new, weight_new, head, *tails, mid = pl.pallas_call(
            kernel,
            name="muon_step",
            out_shape=(
                jax.ShapeDtypeStruct((MATS,) + block, F32),
                jax.ShapeDtypeStruct((MATS,) + block, F32),
                jax.ShapeDtypeStruct((HEAD, 4) + block, BF16),
            )
            + tuple(jax.ShapeDtypeStruct((n, rows, CB), BF16) for _, n, _, rows in TAILS)
            + (jax.ShapeDtypeStruct((1,) + block, BF16),),
            in_specs=[hbm] * 4 + [pl.BlockSpec(memory_space=pltpu.SMEM)],
            out_specs=[hbm] * (4 + len(TAILS)),
            scratch_shapes=[
                pltpu.SMEM((MATS,), F32),
                dma((1,)),
                pltpu.VMEM((2, 2) + block, F32),
                pltpu.VMEM((A_SLOTS, 2) + block, F32),
                pltpu.VMEM((LAG,) + block, F32),
                pltpu.VMEM((B_SLOTS,) + block, F32),
                pltpu.VMEM((LAG,) + block, F32),
                pltpu.VMEM((2,) + block, F32),
                pltpu.VMEM((2,) + block, F32),
                pltpu.VMEM((2,) + block, F32),
                pltpu.VMEM((2,) + block, F32),
                pltpu.VMEM((DEVS,) + block, BF16),
                pltpu.VMEM((DEVS,) + block, BF16),
                pltpu.VMEM((ROUNDS, ROWS, COLS), BF16),
                pltpu.VMEM((MATS,) + block, BF16),
                pltpu.VMEM((COLS, COLS), BF16),
                pltpu.VMEM((COLS, COLS), BF16),
                dma((1,)), dma((LAST + 1,)), dma((LAST + 1,)),
                dma((2,)), dma((A_SLOTS,)), dma((A_SLOTS,)), dma((LAG,)), dma((B_SLOTS,)),
                dma((2,)), dma((2,)), dma((2,)), dma((2,)),
                dma((DEVS,)), dma((MATS,)), dma((MATS,)), dma((MATS,)),
                dma((DEVS,)), dma((DEVS,)), dma((DEVS,)), dma((MATS,)), dma((MATS,)),
                dma((MATS,)), dma((MATS,)),
            ],
            compiler_params=pltpu.CompilerParams(
                collective_id=0, has_side_effects=True, vmem_limit_bytes=67_000_000
            ),
            cost_estimate=pl.CostEstimate(
                flops=3 * 28_700_000_000, bytes_accessed=400_000_000, transcendentals=0
            ),
        )(
            grad_local.reshape((MATS, 2, 2) + block),
            mom_local,
            weight_local,
            learn_rate,
            decay_rate,
        )
        across = [(0, 2), (1, 3), (2, 0), (3, 1)]
        beside = [(0, 1), (1, 0), (2, 3), (3, 2)]

        def move(value, pairs):
            return lax.ppermute(value, "dp", pairs)

        nbr = [mid] + [move(tails[n], across) for n in range(1, len(tails))]
        par = [move(part, beside) for part in tails]
        fwd = [move(part, beside) for part in nbr]
        mom_new, weight_new, full = publish(mom_new, weight_new, head)
        full = full.reshape((MATS, 4) + block)
        for n, part in enumerate(tails):
            full = fill(full, TAILS[n], part, par[n], nbr[n], fwd[n])
        return (
            mom_new.reshape((MATS,) + block),
            weight_new.reshape((MATS,) + block),
            full.reshape(MATS, ROWS, CB),
        )

    return jax.shard_map(
        local_step,
        mesh=mesh,
        in_specs=(P(("rep", "dp"), None, None, "tp"), P("rep", "dp", "tp"), P("rep", "dp", "tp"), P("rep"), P()),
        out_specs=(P("rep", "dp", "tp"), P("rep", "dp", "tp"), P("rep", None, "tp")),
        check_vma=False,
    )
```
